256 devices in a mesh: groups: 4 (over x, y), gx: 64 (over z, core).
Axes of the slice: x: 2, y: 2, z: 32, core: 2. Of those that a mesh axis runs over, the one named last changes fastest.
The devices are a block of a 4x8x32 slice.
Arguments:
- positions: float32 [3, 1048576], P(None, ('groups', 'gx')), parts along dimension 1, may hold values from -0.08 to 127.08, as said below
- radii: float32 [1048576], P(('groups', 'gx')), parts along dimension 0, may hold values from 0.5 to 0.56
- neighbours: int32 [6, 1048576], P(None, ('groups', 'gx')), parts along dimension 1, may hold values from 0 to 262143, as said below
- right_side: float32 [3, 1048576], P(None, ('groups', 'gx')), parts along dimension 1, may hold values from -6 to 6
Outputs:
- solution_field: float32 [3, 1048576], P(None, ('groups', 'gx')), parts along dimension 1
- residual: float32 [3, 1048576], P(None, ('groups', 'gx')), parts along dimension 1
The draws below stay inside these ranges and needn't reach their ends.
There are 4 independent parts, one for each index of `groups`. The reference program is written for one: setup_inputs(seed, part) draws one part's arguments, and reference() takes and returns one part's arrays. A program takes and returns all parts, laid end to end along the dimension named above; each array names one. Nothing has to cross between parts.
Inputs may be any that keep to these rules, and one draw needn't show every extreme that they name: `positions`: particles are ordered by lattice planes of 2048 along the first coordinate, rows of 128 within a plane; each lies within 0.08 of its lattice site in every coordinate. `neighbours`: each column lists distinct partners of the particle, the other slots hold the particle's own index; partnership is symmetric; every partner index is the particle's index plus or minus 1, 128 or 2048.
All inputs are finite; a program needn't handle non-finite values.
Results may differ from the reference program's by a relative error of at most 0.0003.
Values sent between devices are 32-bit elements; how exact they have to be, the bound alone decides.
No kernel may reach another device: no remote copies, remote signals or barrier semaphores. Data moves between devices by JAX's collectives and lax.ppermute only.
A program may use at most 64 MiB of HBM per device.

```python
import jax
import jax.numpy as jnp
from jax import lax

LY = 16
LZ = 128
ITERS = 4
LX = 128
PARTICLES = 262144


def lattice_sites():
    particle_ids = jnp.arange(PARTICLES, dtype=jnp.int32)
    first = particle_ids // (LY * LZ)
    second = particle_ids // LZ % LY
    third = particle_ids % LZ
    return (particle_ids, first, second, third)


def draw_positions(key, part):
    particle_ids, first, second, third = lattice_sites()
    sites = jnp.stack([first, second, third], axis=0).astype(jnp.float32)
    jitter = jnp.clip(0.03 * jax.random.normal(key, (3, PARTICLES), jnp.float32), -0.08, 0.08)
    return sites + jitter


def draw_neighbours(key, part):
    particle_ids, first, second, third = lattice_sites()
    plane_size = LY * LZ
    bonds = jax.random.randint(jax.random.fold_in(key, 11), (3, PARTICLES), 0, 5) > 0
    bond_first = bonds[0] & (first < LX - 1)
    bond_second = bonds[1] & (second < LY - 1)
    bond_third = bonds[2] & (third < LZ - 1)
    back_first = jnp.roll(bond_first, plane_size) & (first > 0)
    back_second = jnp.roll(bond_second, LZ) & (second > 0)
    back_third = jnp.roll(bond_third, 1) & (third > 0)
    slots = jnp.stack([jnp.where(bond_first, particle_ids + plane_size, particle_ids), jnp.where(back_first, particle_ids - plane_size, particle_ids), jnp.where(bond_second, particle_ids + LZ, particle_ids), jnp.where(back_second, particle_ids - LZ, particle_ids), jnp.where(bond_third, particle_ids + 1, particle_ids), jnp.where(back_third, particle_ids - 1, particle_ids)], axis=0)
    scores = jax.random.randint(jax.random.fold_in(key, 12), (6, PARTICLES), 0, 1048576) * 8
    scores = scores + jnp.arange(6, dtype=jnp.int32)[:, None]
    order = jnp.argsort(scores, axis=0)
    return jnp.take_along_axis(slots, order, axis=0).astype(jnp.int32)


def draw_right_side(key, part):
    particle_ids, first, second, third = lattice_sites()
    ramp = 0.5 + first.astype(jnp.float32) / (LX - 1)
    values = jnp.clip(jax.random.normal(key, (3, PARTICLES), jnp.float32), -4.0, 4.0) * ramp[None, :]
    return values.astype(jnp.float32)


def levels(stream_key, extent, cuts, least, top_value):
    level = 1.0
    for position, shards_of in cuts:
        heights = jax.random.uniform(jax.random.fold_in(jax.random.fold_in(stream_key, 6), position), (shards_of,), jnp.float32, least / len(cuts), top_value / len(cuts))
        level = level * jnp.repeat(jnp.exp(heights), extent[position] // shards_of).reshape((-1,) + (1,) * (len(extent) - 1 - position))
    return level


def setup_inputs(seed: int = 0, part: int = 0) -> dict:
    keys = jax.random.split(jax.random.key(seed), 5)
    own_keys = jax.random.split(jax.random.fold_in(keys[4], part), 5)
    positions = draw_positions(jax.random.fold_in(jax.random.fold_in(keys[4], part), 71), part)
    radii = jnp.clip(0.5 + 0.060000002 * jax.random.uniform(own_keys[1], (PARTICLES,), jnp.float32) ** levels(own_keys[1], (PARTICLES,), ((0, 64),), -0.2, 0.2), 0.5, 0.56)
    neighbours = draw_neighbours(jax.random.fold_in(jax.random.fold_in(keys[4], part), 71), part)
    right_side = draw_right_side(jax.random.fold_in(jax.random.fold_in(keys[4], part), 71), part)
    return dict(positions=positions, radii=radii, neighbours=neighbours, right_side=right_side)


diagonal_shift = 4.0

def pair_terms(own_geom, ext_geom, local_index, present):
    partner = jnp.take(ext_geom[:3], local_index, axis=1)
    offset = partner - own_geom[:3][:, None, :]
    squared = lax.optimization_barrier(jnp.sum(offset * offset, axis=0))
    distance = jnp.sqrt(jnp.where(present, squared, jnp.float32(1.0)))
    normal = offset / distance
    contact = own_geom[3][None, :] + jnp.take(ext_geom[3], local_index, axis=0)
    stiffness = 1.0 / (contact * contact)
    tension = -(1.0 - distance / contact) / (contact * distance)
    live_mask = present.astype(jnp.float32)
    return (normal, tension * live_mask, (stiffness - tension) * live_mask)

def apply_terms(vector, extended, local_index, blocks):
    normal, tension, radial = blocks
    partner = jnp.take(extended, local_index, axis=1)
    relative = vector[:, None, :] - partner
    along_normal = lax.optimization_barrier(jnp.sum(normal * relative, axis=0))
    return diagonal_shift * vector + lax.optimization_barrier(jnp.sum(tension * relative + radial * normal * along_normal, axis=1))

def reference(positions, radii, neighbours, right_side):
    owned = positions.shape[1]
    particle_ids = jnp.arange(owned, dtype=jnp.int32)
    present = neighbours != particle_ids[None, :]
    geometry = jnp.concatenate([positions, radii[None, :]], axis=0)
    blocks = pair_terms(geometry, geometry, neighbours, present)
    solution_field = jnp.zeros_like(right_side)
    residual = right_side
    direction = right_side
    norm_now = jnp.sum(residual * residual)
    for iteration in range(ITERS):
        image_vec = apply_terms(direction, direction, neighbours, blocks)
        step_size = norm_now / jnp.sum(direction * image_vec)
        solution_field = solution_field + step_size * direction
        residual = residual - step_size * image_vec
        norm_next = jnp.sum(residual * residual)
        direction = residual + norm_next / norm_now * direction
        norm_now = norm_next
    return (solution_field, residual)
```

```python
import jax
import jax.numpy as jnp
from jax import lax
from jax.experimental import pallas as pl
from jax.experimental.pallas import tpu as pltpu
from jax.sharding import PartitionSpec as P

LY = 16
LZ = 128
ITERS = 4
DIAGONAL_SHIFT = 4.0

CENTER = 5.7
RADIUS = 2.3
ORIGIN = -CENTER / RADIUS
MOMENTS = 2 * ITERS
LOWEST, HIGHEST = -2.2, 4.6

f32 = jnp.float32


def second_kind(order):
    below, value = 0.0, 1.0
    for _ in range(order):
        below, value = value, 2.0 * ORIGIN * value - below
    return value


def pack_kernel(first_ref, pos_ref, rad_ref, nb_ref, rhs_ref, out_ref):
    rows = rad_ref.shape[0]
    shape = (rows, LZ)
    ids = first_ref[0] + (
        lax.broadcasted_iota(jnp.int32, shape, 0) * LZ
        + lax.broadcasted_iota(jnp.int32, shape, 1)
    )
    for c in range(3):
        out_ref[c] = pos_ref[:, c, :]
        out_ref[7 + c] = rhs_ref[:, c, :]
    out_ref[3] = rad_ref[...]
    slots = [nb_ref[:, s, :] - ids for s in range(nb_ref.shape[1])]
    for b, shift in enumerate((LY * LZ, LZ, 1)):
        hit = slots[0] == shift
        for other in slots[1:]:
            hit = hit | (other == shift)
        out_ref[4 + b] = jnp.where(hit, f32(1.0), f32(0.0))


def up_row(x):
    return pltpu.roll(x, x.shape[0] - 1, 0)


def down_row(x):
    return pltpu.roll(x, 1, 0)


def next_lane(x, x_up, lane):
    return pltpu.roll(jnp.where(lane == 0, x_up, x), LZ - 1, 1)


def bond(mask, delta, contact):
    squared = delta[0] * delta[0] + delta[1] * delta[1] + delta[2] * delta[2]
    live = mask > 0.5
    squared = jnp.where(live, squared, f32(1.0))
    inverse = 1.0 / (contact * jnp.sqrt(squared))
    tension = (squared * inverse - 1.0) * inverse
    over = inverse * contact
    weight = jnp.sqrt(inverse) * over
    tension = jnp.where(live, tension, f32(0.0))
    weight = jnp.where(live, weight, f32(0.0))
    return tension, [d * weight for d in delta]


def flux(pair, here, there):
    tension, w = pair
    rel = [a - b for a, b in zip(here, there)]
    along = w[0] * rel[0] + w[1] * rel[1] + w[2] * rel[2]
    return [tension * r + along * n for r, n in zip(rel, w)]


def cut(values, lo, hi):
    return [v[lo:hi] for v in values]


def krylov_kernel(ll_ref, l_ref, own_ref, r_ref, rr_ref, basis_ref, sums_ref):
    rows = own_ref.shape[1]
    depth = 2 * rows
    total = rows + 2 * depth

    def ext(c):
        return jnp.concatenate(
            [ref[c] for ref in (ll_ref, l_ref, own_ref, r_ref, rr_ref)], axis=0
        )

    lane = lax.broadcasted_iota(jnp.int32, (total, LZ), 1)
    geom = [ext(c) for c in range(4)]
    masks = [ext(4 + c) for c in range(3)]
    vector = [ext(7 + c) for c in range(3)]

    ahead = [g[LY:] for g in geom]
    base = [g[: total - LY] for g in geom]
    bond_x = bond(
        masks[0][: total - LY],
        [a - b for a, b in zip(ahead[:3], base[:3])],
        ahead[3] + base[3],
    )
    ups = [up_row(g) for g in geom]
    bond_y = bond(masks[1], [a - b for a, b in zip(ups[:3], geom[:3])], ups[3] + geom[3])
    nexts = [next_lane(g, u, lane) for g, u in zip(geom, ups)]
    bond_z = bond(
        masks[2], [a - b for a, b in zip(nexts[:3], geom[:3])], nexts[3] + geom[3]
    )

    def pair_at(pair, lo, hi):
        return pair[0][lo:hi], cut(pair[1], lo, hi)

    def operate(v, lo, hi):
        n = hi - lo
        here = cut(v, 0, n - LY)
        fx = flux(pair_at(bond_x, lo, hi - LY), here, cut(v, LY, n))
        a, b = lo + 8, hi - 8
        mid = cut(v, 8, n - 8)
        up = [x[8 : n - 8] for x in (up_row(x) for x in v)]
        ln = lane[: b - a]
        fy = flux(pair_at(bond_y, a, b), mid, up)
        nxt = [next_lane(x, u, ln) for x, u in zip(mid, up)]
        fz = flux(pair_at(bond_z, a, b), mid, nxt)
        result = []
        m = n - 2 * LY
        for c in range(3):
            rolled = pltpu.roll(fz[c], 1, 1)
            first = ln == 0
            back = down_row(fy[c] + jnp.where(first, rolled, f32(0.0)))
            side = fy[c] + fz[c] - back - jnp.where(first, f32(0.0), rolled)
            straight = fx[c][LY : LY + m] - fx[c][:m]
            result.append(
                f32(DIAGONAL_SHIFT - CENTER) * v[c][LY : LY + m]
                + straight
                + side[8 : 8 + m]
            )
        return result

    own = slice(depth, depth + rows)
    kept = [[x[own] for x in vector]]
    lo, hi = 0, total
    before, now = None, vector
    for k in range(ITERS):
        image = operate(now, lo, hi)
        m = hi - lo - 2 * LY
        if k == 0:
            after = [x * f32(1.0 / RADIUS) for x in image]
        else:
            after = [
                x * f32(2.0 / RADIUS) - p[2 * LY : 2 * LY + m]
                for x, p in zip(image, before)
            ]
        before, now = now, after
        lo, hi = lo + LY, hi - LY
        kept.append([x[depth - lo : depth - lo + rows] for x in now])
    for k in range(ITERS + 1):
        for c in range(3):
            basis_ref[3 * k + c] = kept[k][c]

    sub = lax.broadcasted_iota(jnp.int32, (8, LZ), 0)
    col = lax.broadcasted_iota(jnp.int32, (8, LZ), 1)
    line = jnp.zeros((8, LZ), f32)
    for k in range(MOMENTS):
        i = k // 2
        j = k - i
        prod = (
            kept[i][0] * kept[j][0] + kept[i][1] * kept[j][1] + kept[i][2] * kept[j][2]
        )
        part = prod[:8]
        for r in range(8, rows, 8):
            part = part + prod[r : r + 8]
        for s in (4, 2, 1):
            part = part + pltpu.roll(part, s, 0)
        line = jnp.where(sub == k, part, line)
    for s in (64, 32, 16):
        line = line + pltpu.roll(line, s, 1)
    line = jnp.where(col // 16 == sub, line, f32(0.0))
    for s in (4, 2, 1):
        line = line + pltpu.roll(line, s, 0)
    sums_ref[...] = jnp.broadcast_to(line[:1][None], sums_ref.shape)


def coefficients(products):
    m = list(products[:2])
    for k in range(2, MOMENTS):
        m.append(2.0 * products[k] - m[k % 2])
    zero = jnp.zeros_like(m[0])
    one = jnp.ones_like(m[0])
    s_before, s = [zero] * MOMENTS, m
    alpha, beta = s[1] / s[0], None
    ratio = alpha
    c_before, c = [zero] * (ITERS + 1), [one] + [zero] * ITERS
    p_before, p = zero, one
    floor = s[0] * f32(1e-12)
    for k in range(ITERS):
        alpha = jnp.clip(alpha, LOWEST, HIGHEST)
        nc = [zero] * (ITERS + 1)
        for l in range(k + 1):
            if l == 0:
                nc[1] = nc[1] + c[0]
            else:
                nc[l - 1] = nc[l - 1] + 0.5 * c[l]
                nc[l + 1] = nc[l + 1] + 0.5 * c[l]
        for l in range(k + 1):
            nc[l] = nc[l] - alpha * c[l]
            if beta is not None and l < k:
                nc[l] = nc[l] - beta * c_before[l]
        np_ = (ORIGIN - alpha) * p
        if beta is not None:
            np_ = np_ - beta * p_before
        if k + 1 < ITERS:
            ns = [zero] * MOMENTS
            for l in range(k + 1, MOMENTS - k - 1):
                ns[l] = 0.5 * (s[l + 1] + s[abs(l - 1)]) - alpha * s[l]
                if beta is not None:
                    ns[l] = ns[l] - beta * s_before[l]
            q = k + 1
            den = jnp.maximum(ns[q], floor)
            factor = 1.0 if q == 1 else 0.5
            next_beta = factor * den / jnp.maximum(s[q - 1], floor)
            new_ratio = ns[q + 1] / den * 0.5
            alpha = new_ratio - ratio
            ratio = new_ratio
            s_before, s = s, ns
            beta = next_beta
        c_before, c = c, nc
        p_before, p = p, np_
    scale = 1.0 / p
    res = [x * scale for x in c]
    sol = []
    for i in range(ITERS):
        total = zero
        for j in range(i + 1, ITERS + 1):
            total = total + res[j] * f32(second_kind(j - 1 - i))
        sol.append(total * f32((-1.0 if i == 0 else -2.0) / RADIUS))
    return res, sol


def finish_kernel(basis_ref, sums_ref, sol_ref, res_ref):
    line = jnp.sum(sums_ref[...], axis=0)
    line = jnp.sum(line, axis=0, keepdims=True)
    line = jnp.broadcast_to(line, (8, LZ))
    for s in (8, 4, 2, 1):
        line = line + pltpu.roll(line, s, 1)
    products = [
        jnp.broadcast_to(line[:, 16 * k + 15 : 16 * k + 16], (8, LZ))
        for k in range(MOMENTS)
    ]
    res, sol = coefficients(products)
    rows = basis_ref.shape[1]
    for c in range(3):
        for r in range(0, rows, 8):
            t = [basis_ref[3 * k + c, r : r + 8, :] for k in range(ITERS + 1)]
            x = sol[0] * t[0]
            for k in range(1, ITERS):
                x = x + sol[k] * t[k]
            y = res[0] * t[0]
            for k in range(1, ITERS + 1):
                y = y + res[k] * t[k]
            sol_ref[r : r + 8, c, :] = x
            res_ref[r : r + 8, c, :] = y


def by_rows(array):
    return array.reshape(array.shape[0], -1, LZ).transpose(1, 0, 2)


def on_device(positions, radii, neighbours, right_side):
    owned = positions.shape[1]
    rows = owned // LZ
    devices = lax.axis_size("gx")
    first = (lax.axis_index("gx") * owned).astype(jnp.int32).reshape(1)
    vmem = pl.BlockSpec(memory_space=pltpu.VMEM)
    smem = pl.BlockSpec(memory_space=pltpu.SMEM)

    packed = pl.pallas_call(
        pack_kernel,
        out_shape=jax.ShapeDtypeStruct((10, rows, LZ), f32),
        in_specs=[smem, vmem, vmem, vmem, vmem],
        out_specs=vmem,
        compiler_params=pltpu.CompilerParams(vmem_limit_bytes=4 << 20),
        name="pack",
    )(
        first,
        by_rows(positions),
        radii.reshape(rows, LZ),
        by_rows(neighbours),
        by_rows(right_side),
    )

    def moved(array, by):
        pairs = [(i, (i + by) % devices) for i in range(devices)]
        return lax.ppermute(array, "gx", pairs)

    left, right = moved(packed, 1), moved(packed, -1)
    far_left, far_right = moved(packed, 2), moved(packed, -2)

    basis, sums = pl.pallas_call(
        krylov_kernel,
        out_shape=(
            jax.ShapeDtypeStruct((3 * (ITERS + 1), rows, LZ), f32),
            jax.ShapeDtypeStruct((devices, 1, LZ), f32),
        ),
        in_specs=[vmem] * 5,
        out_specs=(vmem, vmem),
        compiler_params=pltpu.CompilerParams(vmem_limit_bytes=12 << 20),
        name="krylov",
    )(far_left, left, packed, right, far_right)

    everyone = lax.all_to_all(sums, "gx", split_axis=0, concat_axis=0, tiled=True)

    sol, res = pl.pallas_call(
        finish_kernel,
        out_shape=(
            jax.ShapeDtypeStruct((rows, 3, LZ), f32),
            jax.ShapeDtypeStruct((rows, 3, LZ), f32),
        ),
        in_specs=[vmem, vmem],
        out_specs=(vmem, vmem),
        compiler_params=pltpu.CompilerParams(vmem_limit_bytes=4 << 20),
        name="finish",
    )(basis, everyone.reshape(-1, 8, LZ))
    back = lambda a: a.transpose(1, 0, 2).reshape(3, owned)
    return back(sol), back(res)


def solution(mesh):
    return jax.shard_map(
        on_device,
        mesh=mesh,
        in_specs=(
            P(None, ("groups", "gx")),
            P(("groups", "gx")),
            P(None, ("groups", "gx")),
            P(None, ("groups", "gx")),
        ),
        out_specs=(P(None, ("groups", "gx")), P(None, ("groups", "gx"))),
        check_vma=False,
    )
```

```python
import jax
import jax.numpy as jnp
from jax import lax
from jax.experimental import pallas as pl
from jax.experimental.pallas import tpu as pltpu
from jax.sharding import PartitionSpec as P

LY = 16
LZ = 128
ITERS = 4
DIAGONAL_SHIFT = 4.0

CENTER = 5.7
RADIUS = 2.3
ORIGIN = -CENTER / RADIUS
MOMENTS = 2 * ITERS
LOWEST, HIGHEST = -2.2, 4.6

f32 = jnp.float32


def second_kind(order):
    below, value = 0.0, 1.0
    for _ in range(order):
        below, value = value, 2.0 * ORIGIN * value - below
    return value


def pack_kernel(first_ref, pos_ref, rad_ref, nb_ref, rhs_ref, out_ref):
    rows = rad_ref.shape[0]
    shape = (rows, LZ)
    ids = first_ref[0] + (
        lax.broadcasted_iota(jnp.int32, shape, 0) * LZ
        + lax.broadcasted_iota(jnp.int32, shape, 1)
    )
    for c in range(3):
        out_ref[c] = pos_ref[:, c, :]
        out_ref[7 + c] = rhs_ref[:, c, :]
    out_ref[3] = rad_ref[...]
    slots = [nb_ref[:, s, :] - ids for s in range(nb_ref.shape[1])]
    for b, shift in enumerate((LY * LZ, LZ, 1)):
        hit = slots[0] == shift
        for other in slots[1:]:
            hit = hit | (other == shift)
        out_ref[4 + b] = jnp.where(hit, f32(1.0), f32(0.0))


def up_row(x):
    return pltpu.roll(x, x.shape[0] - 1, 0)


def down_row(x):
    return pltpu.roll(x, 1, 0)


def next_lane(x, x_up, lane):
    return pltpu.roll(jnp.where(lane == 0, x_up, x), LZ - 1, 1)


def bond(mask, delta, contact):
    squared = delta[0] * delta[0] + delta[1] * delta[1] + delta[2] * delta[2]
    live = mask > 0.5
    squared = jnp.where(live, squared, f32(1.0))
    inverse = 1.0 / (contact * jnp.sqrt(squared))
    tension = (squared * inverse - 1.0) * inverse
    over = inverse * contact
    weight = jnp.sqrt(inverse) * over
    tension = jnp.where(live, tension, f32(0.0))
    weight = jnp.where(live, weight, f32(0.0))
    return tension, [d * weight for d in delta]


def flux(pair, here, there):
    tension, w = pair
    rel = [a - b for a, b in zip(here, there)]
    along = w[0] * rel[0] + w[1] * rel[1] + w[2] * rel[2]
    return [tension * r + along * n for r, n in zip(rel, w)]


def cut(values, lo, hi):
    return [v[lo:hi] for v in values]


def krylov_kernel(ll_ref, l_ref, own_ref, r_ref, rr_ref, basis_ref, sums_ref):
    rows = own_ref.shape[1]
    depth = 2 * rows
    total = rows + 2 * depth

    def ext(c):
        return jnp.concatenate(
            [ref[c] for ref in (ll_ref, l_ref, own_ref, r_ref, rr_ref)], axis=0
        )

    lane = lax.broadcasted_iota(jnp.int32, (total, LZ), 1)
    geom = [ext(c) for c in range(4)]
    masks = [ext(4 + c) for c in range(3)]
    vector = [ext(7 + c) for c in range(3)]

    ahead = [g[LY:] for g in geom]
    base = [g[: total - LY] for g in geom]
    bond_x = bond(
        masks[0][: total - LY],
        [a - b for a, b in zip(ahead[:3], base[:3])],
        ahead[3] + base[3],
    )
    ups = [up_row(g) for g in geom]
    bond_y = bond(masks[1], [a - b for a, b in zip(ups[:3], geom[:3])], ups[3] + geom[3])
    nexts = [next_lane(g, u, lane) for g, u in zip(geom, ups)]
    bond_z = bond(
        masks[2], [a - b for a, b in zip(nexts[:3], geom[:3])], nexts[3] + geom[3]
    )

    def pair_at(pair, lo, hi):
        return pair[0][lo:hi], cut(pair[1], lo, hi)

    def operate(v, lo, hi):
        n = hi - lo
        here = cut(v, 0, n - LY)
        fx = flux(pair_at(bond_x, lo, hi - LY), here, cut(v, LY, n))
        a, b = lo + 8, hi - 8
        mid = cut(v, 8, n - 8)
        up = [x[8 : n - 8] for x in (up_row(x) for x in v)]
        ln = lane[: b - a]
        fy = flux(pair_at(bond_y, a, b), mid, up)
        nxt = [next_lane(x, u, ln) for x, u in zip(mid, up)]
        fz = flux(pair_at(bond_z, a, b), mid, nxt)
        result = []
        m = n - 2 * LY
        for c in range(3):
            rolled = pltpu.roll(fz[c], 1, 1)
            first = ln == 0
            back = down_row(fy[c] + jnp.where(first, rolled, f32(0.0)))
            side = fy[c] + fz[c] - back - jnp.where(first, f32(0.0), rolled)
            straight = fx[c][LY : LY + m] - fx[c][:m]
            result.append(
                f32(DIAGONAL_SHIFT - CENTER) * v[c][LY : LY + m]
                + straight
                + side[8 : 8 + m]
            )
        return result

    own = slice(depth, depth + rows)
    kept = [[x[own] for x in vector]]
    lo, hi = 0, total
    before, now = None, vector
    for k in range(ITERS):
        image = operate(now, lo, hi)
        m = hi - lo - 2 * LY
        if k == 0:
            after = [x * f32(1.0 / RADIUS) for x in image]
        else:
            after = [
                x * f32(2.0 / RADIUS) - p[2 * LY : 2 * LY + m]
                for x, p in zip(image, before)
            ]
        before, now = now, after
        lo, hi = lo + LY, hi - LY
        kept.append([x[depth - lo : depth - lo + rows] for x in now])
    for k in range(ITERS + 1):
        for c in range(3):
            basis_ref[3 * k + c] = kept[k][c]

    sub = lax.broadcasted_iota(jnp.int32, (8, LZ), 0)
    col = lax.broadcasted_iota(jnp.int32, (8, LZ), 1)
    line = jnp.zeros((8, LZ), f32)
    for k in range(MOMENTS):
        i = k // 2
        j = k - i
        prod = (
            kept[i][0] * kept[j][0] + kept[i][1] * kept[j][1] + kept[i][2] * kept[j][2]
        )
        part = prod[:8]
        for r in range(8, rows, 8):
            part = part + prod[r : r + 8]
        for s in (4, 2, 1):
            part = part + pltpu.roll(part, s, 0)
        line = jnp.where(sub == k, part, line)
    for s in (64, 32, 16):
        line = line + pltpu.roll(line, s, 1)
    line = jnp.where(col // 16 == sub, line, f32(0.0))
    for s in (4, 2, 1):
        line = line + pltpu.roll(line, s, 0)
    sums_ref[...] = jnp.broadcast_to(line[:1][None], sums_ref.shape)


def coefficients(products):
    m = list(products[:2])
    for k in range(2, MOMENTS):
        m.append(2.0 * products[k] - m[k % 2])
    zero = jnp.zeros_like(m[0])
    one = jnp.ones_like(m[0])
    s_before, s = [zero] * MOMENTS, m
    alpha, beta = s[1] / s[0], None
    ratio = alpha
    c_before, c = [zero] * (ITERS + 1), [one] + [zero] * ITERS
    p_before, p = zero, one
    floor = s[0] * f32(1e-12)
    for k in range(ITERS):
        alpha = jnp.clip(alpha, LOWEST, HIGHEST)
        nc = [zero] * (ITERS + 1)
        for l in range(k + 1):
            if l == 0:
                nc[1] = nc[1] + c[0]
            else:
                nc[l - 1] = nc[l - 1] + 0.5 * c[l]
                nc[l + 1] = nc[l + 1] + 0.5 * c[l]
        for l in range(k + 1):
            nc[l] = nc[l] - alpha * c[l]
            if beta is not None and l < k:
                nc[l] = nc[l] - beta * c_before[l]
        np_ = (ORIGIN - alpha) * p
        if beta is not None:
            np_ = np_ - beta * p_before
        if k + 1 < ITERS:
            ns = [zero] * MOMENTS
            for l in range(k + 1, MOMENTS - k - 1):
                ns[l] = 0.5 * (s[l + 1] + s[abs(l - 1)]) - alpha * s[l]
                if beta is not None:
                    ns[l] = ns[l] - beta * s_before[l]
            q = k + 1
            den = jnp.maximum(ns[q], floor)
            factor = 1.0 if q == 1 else 0.5
            next_beta = factor * den / jnp.maximum(s[q - 1], floor)
            new_ratio = ns[q + 1] / den * 0.5
            alpha = new_ratio - ratio
            ratio = new_ratio
            s_before, s = s, ns
            beta = next_beta
        c_before, c = c, nc
        p_before, p = p, np_
    scale = 1.0 / p
    res = [x * scale for x in c]
    sol = []
    for i in range(ITERS):
        total = zero
        for j in range(i + 1, ITERS + 1):
            total = total + res[j] * f32(second_kind(j - 1 - i))
        sol.append(total * f32((-1.0 if i == 0 else -2.0) / RADIUS))
    return res, sol


def finish_kernel(basis_ref, sums_ref, sol_ref, res_ref):
    line = jnp.sum(sums_ref[...], axis=0)
    line = jnp.sum(line, axis=0, keepdims=True)
    line = jnp.broadcast_to(line, (8, LZ))
    for s in (8, 4, 2, 1):
        line = line + pltpu.roll(line, s, 1)
    products = [
        jnp.broadcast_to(line[:, 16 * k + 15 : 16 * k + 16], (8, LZ))
        for k in range(MOMENTS)
    ]
    res, sol = coefficients(products)
    rows = basis_ref.shape[1]
    for c in range(3):
        for r in range(0, rows, 8):
            t = [basis_ref[3 * k + c, r : r + 8, :] for k in range(ITERS + 1)]
            x = sol[0] * t[0]
            for k in range(1, ITERS):
                x = x + sol[k] * t[k]
            y = res[0] * t[0]
            for k in range(1, ITERS + 1):
                y = y + res[k] * t[k]
            sol_ref[r : r + 8, c, :] = x
            res_ref[r : r + 8, c, :] = y


def by_rows(array):
    return array.reshape(array.shape[0], -1, LZ).transpose(1, 0, 2)


def on_device(positions, radii, neighbours, right_side):
    owned = positions.shape[1]
    rows = owned // LZ
    devices = lax.axis_size("gx")
    first = (lax.axis_index("gx") * owned).astype(jnp.int32).reshape(1)
    vmem = pl.BlockSpec(memory_space=pltpu.VMEM)
    smem = pl.BlockSpec(memory_space=pltpu.SMEM)

    packed = pl.pallas_call(
        pack_kernel,
        out_shape=jax.ShapeDtypeStruct((10, rows, LZ), f32),
        in_specs=[smem, vmem, vmem, vmem, vmem],
        out_specs=vmem,
        compiler_params=pltpu.CompilerParams(vmem_limit_bytes=4 << 20),
        name="pack",
    )(
        first,
        by_rows(positions),
        radii.reshape(rows, LZ),
        by_rows(neighbours),
        by_rows(right_side),
    )

    def moved(array, by):
        pairs = [(i, (i + by) % devices) for i in range(devices)]
        return lax.ppermute(array, "gx", pairs)

    left, right = moved(packed, 1), moved(packed, -1)
    far_left, far_right = moved(packed, 2), moved(packed, -2)

    basis, sums = pl.pallas_call(
        krylov_kernel,
        out_shape=(
            jax.ShapeDtypeStruct((3 * (ITERS + 1), rows, LZ), f32),
            jax.ShapeDtypeStruct((devices, 1, LZ), f32),
        ),
        in_specs=[vmem] * 5,
        out_specs=(vmem, vmem),
        compiler_params=pltpu.CompilerParams(vmem_limit_bytes=12 << 20),
        name="krylov",
    )(far_left, left, packed, right, far_right)

    order = [(i + devices // 2) % devices for i in range(devices)]
    everyone = lax.all_to_all(
        sums, "gx", split_axis=0, concat_axis=0, tiled=True, axis_index_groups=[order]
    )

    sol, res = pl.pallas_call(
        finish_kernel,
        out_shape=(
            jax.ShapeDtypeStruct((rows, 3, LZ), f32),
            jax.ShapeDtypeStruct((rows, 3, LZ), f32),
        ),
        in_specs=[vmem, vmem],
        out_specs=(vmem, vmem),
        compiler_params=pltpu.CompilerParams(vmem_limit_bytes=4 << 20),
        name="finish",
    )(basis, everyone.reshape(-1, 8, LZ))
    back = lambda a: a.transpose(1, 0, 2).reshape(3, owned)
    return back(sol), back(res)


def solution(mesh):
    return jax.shard_map(
        on_device,
        mesh=mesh,
        in_specs=(
            P(None, ("groups", "gx")),
            P(("groups", "gx")),
            P(None, ("groups", "gx")),
            P(None, ("groups", "gx")),
        ),
        out_specs=(P(None, ("groups", "gx")), P(None, ("groups", "gx"))),
        check_vma=False,
    )
```

```python
import jax
import jax.numpy as jnp
from jax import lax
from jax.experimental import pallas as pl
from jax.experimental.pallas import tpu as pltpu
from jax.sharding import PartitionSpec as P

LY = 16
LZ = 128
ITERS = 4
DIAGONAL_SHIFT = 4.0

CENTER = 5.7
RADIUS = 2.3
ORIGIN = -CENTER / RADIUS
MOMENTS = 2 * ITERS
LOWEST, HIGHEST = -2.2, 4.6

f32 = jnp.float32


def second_kind(order):
    below, value = 0.0, 1.0
    for _ in range(order):
        below, value = value, 2.0 * ORIGIN * value - below
    return value


def pack_kernel(first_ref, pos_hbm, rad_hbm, nb_hbm, rhs_hbm, out_ref, *scratch):
    pos_ref, rad_ref, nb_ref, rhs_ref, sems = scratch
    moves = [
        pltpu.make_async_copy(src, dst, sems.at[k])
        for k, (src, dst) in enumerate(
            (
                (nb_hbm, nb_ref),
                (pos_hbm, pos_ref),
                (rhs_hbm, rhs_ref),
                (rad_hbm, rad_ref),
            )
        )
    ]
    for move in moves:
        move.start()
    rows = rad_ref.shape[0]
    shape = (rows, LZ)
    ids = first_ref[0] + (
        lax.broadcasted_iota(jnp.int32, shape, 0) * LZ
        + lax.broadcasted_iota(jnp.int32, shape, 1)
    )
    for move in moves:
        move.wait()
    slots = [nb_ref[:, s, :] - ids for s in range(nb_ref.shape[1])]
    for b, shift in enumerate((LY * LZ, LZ, 1)):
        hit = slots[0] == shift
        for other in slots[1:]:
            hit = hit | (other == shift)
        out_ref[4 + b] = jnp.where(hit, f32(1.0), f32(0.0))
    for c in range(3):
        out_ref[c] = pos_ref[:, c, :]
        out_ref[7 + c] = rhs_ref[:, c, :]
    out_ref[3] = rad_ref[...]


def edge_kernel(own_ref, low_ref, high_ref):
    rows = own_ref.shape[1]
    row, lane = coordinates(rows)
    geom = [own_ref[c] for c in range(4)]
    inside = row < rows - 1
    last = (row == rows - 1) & (lane == LZ - 1)
    vector = [own_ref[7 + c] for c in range(3)]
    bonds = all_bonds(
        geom,
        [own_ref[4], own_ref[5], own_ref[6]],
        lane,
        (None, inside, jnp.logical_not(last)),
    )
    push = fluxes(bonds, vector, lane, 0, rows)
    for c in range(3):
        low_ref[c] = geom[c][:LY]
        high_ref[c] = geom[c][rows - LY :]
        low_ref[4 + c] = vector[c][:LY]
        high_ref[4 + c] = vector[c][rows - LY :]
        low_ref[7 + c] = push[c][:LY]
        high_ref[7 + c] = push[c][rows - LY :]
    low_ref[3] = geom[3][:LY]
    high_ref[3] = geom[3][rows - LY :]
    high_ref[10] = own_ref[4, rows - LY :, :]
    high_ref[11, : LY // 2, :] = own_ref[5, rows - LY // 2 :, :]
    high_ref[11, LY // 2 :, :] = own_ref[6, rows - LY // 2 :, :]


def coordinates(rows):
    shape = (rows, LZ)
    return (
        lax.broadcasted_iota(jnp.int32, shape, 0),
        lax.broadcasted_iota(jnp.int32, shape, 1),
    )


def up_row(x):
    return pltpu.roll(x, x.shape[0] - 1, 0)


def down_row(x):
    return pltpu.roll(x, 1, 0)


def next_lane(x, x_up, lane):
    return pltpu.roll(jnp.where(lane == 0, x_up, x), LZ - 1, 1)


def bond(mask, delta, contact, allowed=None):
    squared = delta[0] * delta[0] + delta[1] * delta[1] + delta[2] * delta[2]
    live = mask > 0.5
    if allowed is not None:
        live = live & allowed
    squared = jnp.where(live, squared, f32(1.0))
    inverse = 1.0 / (contact * jnp.sqrt(squared))
    tension = (squared * inverse - 1.0) * inverse
    over = inverse * contact
    weight = jnp.sqrt(inverse) * over
    tension = jnp.where(live, tension, f32(0.0))
    weight = jnp.where(live, weight, f32(0.0))
    return tension, [d * weight for d in delta]


def all_bonds(geom, masks, lane, allowed=(None, None, None)):
    total = geom[0].shape[0]
    ahead = [g[LY:] for g in geom]
    base = [g[: total - LY] for g in geom]
    ups = [up_row(g) for g in geom]
    nexts = [next_lane(g, u, lane) for g, u in zip(geom, ups)]

    def build(mask, there, here, ok):
        delta = [a - b for a, b in zip(there[:3], here[:3])]
        return bond(mask, delta, there[3] + here[3], ok)

    return (
        build(masks[0][: total - LY], ahead, base, allowed[0]),
        build(masks[1], ups, geom, allowed[1]),
        build(masks[2], nexts, geom, allowed[2]),
    )


def flux(pair, here, there):
    tension, w = pair
    rel = [a - b for a, b in zip(here, there)]
    along = w[0] * rel[0] + w[1] * rel[1] + w[2] * rel[2]
    return [tension * r + along * n for r, n in zip(rel, w)]


def cut(values, lo, hi):
    return [v[lo:hi] for v in values]


def cut_pair(pair, lo, hi):
    return pair[0][lo:hi], cut(pair[1], lo, hi)


def side_flux(bonds, mid, up, lane, lo, hi):
    fy = flux(cut_pair(bonds[1], lo, hi), mid, up)
    nxt = [next_lane(x, u, lane) for x, u in zip(mid, up)]
    fz = flux(cut_pair(bonds[2], lo, hi), mid, nxt)
    first = lane == 0
    result = []
    for y, z in zip(fy, fz):
        rolled = pltpu.roll(z, 1, 1)
        back = down_row(y + jnp.where(first, rolled, f32(0.0)))
        result.append(y + z - back - jnp.where(first, f32(0.0), rolled))
    return result


def fluxes(bonds, v, lane, lo, hi):
    n = hi - lo
    fx = flux(cut_pair(bonds[0], lo, hi - LY), cut(v, 0, n - LY), cut(v, LY, n))
    side = side_flux(bonds, v, [up_row(x) for x in v], lane[:n], lo, hi)
    result = []
    for s, x in zip(side, fx):
        parts = [x[:LY], -x[n - 2 * LY :]]
        if n > 2 * LY:
            parts.insert(1, x[LY:] - x[: n - 2 * LY])
        result.append(s + jnp.concatenate(parts, axis=0))
    return result


def krylov_kernel(ll_ref, l_ref, own_ref, r_ref, rr_ref, basis_ref, sums_ref):
    rows = own_ref.shape[1]
    depth = rows + LY
    total = rows + 2 * depth
    row, lane = coordinates(total)
    half = LY // 2

    def ext(c, low, high):
        return jnp.concatenate(
            [low] + [ref[c] for ref in (l_ref, own_ref, r_ref)] + [high], axis=0
        )

    none = jnp.zeros((LY, LZ), f32)
    pad = jnp.zeros((LY - half, LZ), f32)
    rim = row == LY - 1
    past = row >= LY
    geom = [ext(c, ll_ref[c], rr_ref[c]) for c in range(4)]
    vector = [ext(7 + c, ll_ref[4 + c], rr_ref[4 + c]) for c in range(3)]
    masks = [
        ext(4, ll_ref[10], none),
        ext(5, jnp.concatenate([pad, ll_ref[11, :half, :]], axis=0), none),
        ext(6, jnp.concatenate([pad, ll_ref[11, half:, :]], axis=0), none),
    ]
    bonds = all_bonds(
        geom, masks, lane, (None, past | rim, past | (rim & (lane == LZ - 1)))
    )

    def operate(v, lo, hi):
        n = hi - lo
        m = n - 2 * LY
        fx = flux(cut_pair(bonds[0], lo, hi - LY), cut(v, 0, n - LY), cut(v, LY, n))
        up = [up_row(x)[8 : n - 8] for x in v]
        side = side_flux(bonds, cut(v, 8, n - 8), up, lane[: n - 16], lo + 8, hi - 8)
        return [
            f32(DIAGONAL_SHIFT) * v[c][LY : LY + m]
            + (fx[c][LY : LY + m] - fx[c][:m])
            + side[c][8 : 8 + m]
            for c in range(3)
        ]

    kept = [cut(vector, depth, depth + rows)]
    push = fluxes(bonds, vector, lane, 0, total)
    lo, hi = 0, total
    before, now = vector, []
    for c in range(3):
        given = jnp.concatenate(
            [ll_ref[7 + c], jnp.zeros((total - 2 * LY, LZ), f32), rr_ref[7 + c]], axis=0
        )
        image = f32(DIAGONAL_SHIFT - CENTER) * vector[c] + push[c] + given
        now.append(image * f32(1.0 / RADIUS))
    kept.append(cut(now, depth, depth + rows))
    for k in range(1, ITERS):
        image = operate(now, lo, hi)
        m = hi - lo - 2 * LY
        after = [
            (x - f32(CENTER) * y[LY : LY + m]) * f32(2.0 / RADIUS) - p
            for x, y, p in zip(image, now, cut(before, LY, LY + m))
        ]
        before, now = cut(now, LY, LY + m), after
        lo, hi = lo + LY, hi - LY
        kept.append(cut(now, depth - lo, depth - lo + rows))
    for k in range(ITERS + 1):
        for c in range(3):
            basis_ref[3 * k + c] = kept[k][c]

    sub = lax.broadcasted_iota(jnp.int32, (8, LZ), 0)
    col = lax.broadcasted_iota(jnp.int32, (8, LZ), 1)
    line = jnp.zeros((8, LZ), f32)
    for k in range(MOMENTS):
        i = k // 2
        j = k - i
        prod = (
            kept[i][0] * kept[j][0] + kept[i][1] * kept[j][1] + kept[i][2] * kept[j][2]
        )
        part = prod[:8]
        for r in range(8, rows, 8):
            part = part + prod[r : r + 8]
        for s in (4, 2, 1):
            part = part + pltpu.roll(part, s, 0)
        line = jnp.where(sub == k, part, line)
    for s in (64, 32, 16):
        line = line + pltpu.roll(line, s, 1)
    line = jnp.where(col // 16 == sub, line, f32(0.0))
    for s in (4, 2, 1):
        line = line + pltpu.roll(line, s, 0)
    sums_ref[...] = jnp.broadcast_to(line[:1][None], sums_ref.shape)


def coefficients(products):
    m = list(products[:2])
    for k in range(2, MOMENTS):
        m.append(2.0 * products[k] - m[k % 2])
    zero = jnp.zeros_like(m[0])
    one = jnp.ones_like(m[0])
    s_before, s = [zero] * MOMENTS, m
    alpha, beta = s[1] / s[0], None
    ratio = alpha
    c_before, c = [zero] * (ITERS + 1), [one] + [zero] * ITERS
    p_before, p = zero, one
    floor = s[0] * f32(1e-12)
    for k in range(ITERS):
        alpha = jnp.clip(alpha, LOWEST, HIGHEST)
        nc = [zero] * (ITERS + 1)
        for l in range(k + 1):
            if l == 0:
                nc[1] = nc[1] + c[0]
            else:
                nc[l - 1] = nc[l - 1] + 0.5 * c[l]
                nc[l + 1] = nc[l + 1] + 0.5 * c[l]
        for l in range(k + 1):
            nc[l] = nc[l] - alpha * c[l]
            if beta is not None and l < k:
                nc[l] = nc[l] - beta * c_before[l]
        np_ = (ORIGIN - alpha) * p
        if beta is not None:
            np_ = np_ - beta * p_before
        if k + 1 < ITERS:
            ns = [zero] * MOMENTS
            for l in range(k + 1, MOMENTS - k - 1):
                ns[l] = 0.5 * (s[l + 1] + s[abs(l - 1)]) - alpha * s[l]
                if beta is not None:
                    ns[l] = ns[l] - beta * s_before[l]
            q = k + 1
            den = jnp.maximum(ns[q], floor)
            factor = 1.0 if q == 1 else 0.5
            next_beta = factor * den / jnp.maximum(s[q - 1], floor)
            new_ratio = ns[q + 1] / den * 0.5
            alpha = new_ratio - ratio
            ratio = new_ratio
            s_before, s = s, ns
            beta = next_beta
        c_before, c = c, nc
        p_before, p = p, np_
    scale = 1.0 / p
    res = [x * scale for x in c]
    sol = []
    for i in range(ITERS):
        total = zero
        for j in range(i + 1, ITERS + 1):
            total = total + res[j] * f32(second_kind(j - 1 - i))
        sol.append(total * f32((-1.0 if i == 0 else -2.0) / RADIUS))
    return res, sol


def finish_kernel(basis_ref, sums_ref, sol_ref, res_ref):
    line = jnp.sum(sums_ref[...], axis=0)
    line = jnp.sum(line, axis=0, keepdims=True)
    line = jnp.broadcast_to(line, (8, LZ))
    for s in (8, 4, 2, 1):
        line = line + pltpu.roll(line, s, 1)
    products = [
        jnp.broadcast_to(line[:, 16 * k + 15 : 16 * k + 16], (8, LZ))
        for k in range(MOMENTS)
    ]
    res, sol = coefficients(products)
    rows = basis_ref.shape[1]
    for c in range(3):
        for r in range(0, rows, 8):
            t = [basis_ref[3 * k + c, r : r + 8, :] for k in range(ITERS + 1)]
            x = sol[0] * t[0]
            for k in range(1, ITERS):
                x = x + sol[k] * t[k]
            y = res[0] * t[0]
            for k in range(1, ITERS + 1):
                y = y + res[k] * t[k]
            sol_ref[r : r + 8, c, :] = x
            res_ref[r : r + 8, c, :] = y


def by_rows(array):
    return array.reshape(array.shape[0], -1, LZ).transpose(1, 0, 2)


def stay(array):
    return pltpu.with_memory_space_constraint(array, pltpu.HBM)


def on_device(positions, radii, neighbours, right_side):
    owned = positions.shape[1]
    rows = owned // LZ
    devices = lax.axis_size("gx")
    first = (lax.axis_index("gx") * owned).astype(jnp.int32).reshape(1)
    vmem = pl.BlockSpec(memory_space=pltpu.VMEM)
    smem = pl.BlockSpec(memory_space=pltpu.SMEM)
    hbm = pl.BlockSpec(memory_space=pltpu.HBM)

    packed = pl.pallas_call(
        pack_kernel,
        out_shape=jax.ShapeDtypeStruct((10, rows, LZ), f32),
        in_specs=[smem, hbm, hbm, hbm, hbm],
        out_specs=vmem,
        scratch_shapes=[
            pltpu.VMEM((rows, 3, LZ), f32),
            pltpu.VMEM((rows, LZ), f32),
            pltpu.VMEM((rows, neighbours.shape[0], LZ), jnp.int32),
            pltpu.VMEM((rows, 3, LZ), f32),
            pltpu.SemaphoreType.DMA((4,)),
        ],
        compiler_params=pltpu.CompilerParams(vmem_limit_bytes=4 << 20),
        name="pack",
    )(
        first,
        stay(by_rows(positions)),
        stay(radii.reshape(rows, LZ)),
        stay(by_rows(neighbours)),
        stay(by_rows(right_side)),
    )

    def moved(array, by):
        pairs = [(i, (i + by) % devices) for i in range(devices)]
        return lax.ppermute(array, "gx", pairs)

    left, right = moved(packed, 1), moved(packed, -1)
    low, high = pl.pallas_call(
        edge_kernel,
        out_shape=(
            jax.ShapeDtypeStruct((10, LY, LZ), f32),
            jax.ShapeDtypeStruct((12, LY, LZ), f32),
        ),
        in_specs=[vmem],
        out_specs=(vmem, vmem),
        compiler_params=pltpu.CompilerParams(vmem_limit_bytes=4 << 20),
        name="edge",
    )(packed)
    far_left, far_right = moved(high, 2), moved(low, -2)

    basis, sums = pl.pallas_call(
        krylov_kernel,
        out_shape=(
            jax.ShapeDtypeStruct((3 * (ITERS + 1), rows, LZ), f32),
            jax.ShapeDtypeStruct((devices, 1, LZ), f32),
        ),
        in_specs=[vmem] * 5,
        out_specs=(vmem, vmem),
        compiler_params=pltpu.CompilerParams(vmem_limit_bytes=12 << 20),
        name="krylov",
    )(far_left, left, packed, right, far_right)

    order = [(i + devices // 2) % devices for i in range(devices)]
    everyone = lax.all_to_all(
        sums, "gx", split_axis=0, concat_axis=0, tiled=True, axis_index_groups=[order]
    )

    sol, res = pl.pallas_call(
        finish_kernel,
        out_shape=(
            jax.ShapeDtypeStruct((rows, 3, LZ), f32),
            jax.ShapeDtypeStruct((rows, 3, LZ), f32),
        ),
        in_specs=[vmem, vmem],
        out_specs=(vmem, vmem),
        compiler_params=pltpu.CompilerParams(vmem_limit_bytes=4 << 20),
        name="finish",
    )(basis, everyone.reshape(-1, 8, LZ))
    back = lambda a: a.transpose(1, 0, 2).reshape(3, owned)
    return back(sol), back(res)


def solution(mesh):
    return jax.shard_map(
        on_device,
        mesh=mesh,
        in_specs=(
            P(None, ("groups", "gx")),
            P(("groups", "gx")),
            P(None, ("groups", "gx")),
            P(None, ("groups", "gx")),
        ),
        out_specs=(P(None, ("groups", "gx")), P(None, ("groups", "gx"))),
        check_vma=False,
    )
```

```python
import jax
import jax.numpy as jnp
from jax import lax
from jax.experimental import pallas as pl
from jax.experimental.pallas import tpu as pltpu
from jax.sharding import PartitionSpec as P


LY = 16
LZ = 128
ITERS = 4
DIAGONAL_SHIFT = 4.0

CENTER = 5.7
RADIUS = 2.3
ORIGIN = -CENTER / RADIUS
MOMENTS = 2 * ITERS
LOWEST, HIGHEST = -2.2, 4.6

f32 = jnp.float32


def second_kind(order):
    below, value = 0.0, 1.0
    for _ in range(order):
        below, value = value, 2.0 * ORIGIN * value - below
    return value


def pack_kernel(first_ref, pos_hbm, rad_hbm, nb_hbm, rhs_hbm, out_ref, *scratch):
    pos_ref, rad_ref, nb_ref, rhs_ref, sems = scratch
    moves = [
        pltpu.make_async_copy(src, dst, sems.at[k])
        for k, (src, dst) in enumerate(
            (
                (nb_hbm, nb_ref),
                (pos_hbm, pos_ref),
                (rhs_hbm, rhs_ref),
                (rad_hbm, rad_ref),
            )
        )
    ]
    for move in moves:
        move.start()
    rows = rad_ref.shape[0]
    shape = (rows, LZ)
    ids = first_ref[0] + (
        lax.broadcasted_iota(jnp.int32, shape, 0) * LZ
        + lax.broadcasted_iota(jnp.int32, shape, 1)
    )
    for move in moves:
        move.wait()
    slots = [nb_ref[:, s, :] - ids for s in range(nb_ref.shape[1])]
    for b, shift in enumerate((LY * LZ, LZ, 1)):
        hit = slots[0] == shift
        for other in slots[1:]:
            hit = hit | (other == shift)
        out_ref[4 + b] = jnp.where(hit, f32(1.0), f32(0.0))
    for c in range(3):
        out_ref[c] = pos_ref[:, c, :]
        out_ref[7 + c] = rhs_ref[:, c, :]
    out_ref[3] = rad_ref[...]


def edge_kernel(own_ref, low_ref, high_ref):
    rows = own_ref.shape[1]
    row, lane = coordinates(rows)
    geom = [own_ref[c] for c in range(4)]
    inside = row < rows - 1
    last = (row == rows - 1) & (lane == LZ - 1)
    vector = [own_ref[7 + c] for c in range(3)]
    bonds = all_bonds(
        geom,
        [own_ref[4], own_ref[5], own_ref[6]],
        lane,
        (None, inside, jnp.logical_not(last)),
    )
    push = fluxes(bonds, vector, lane, 0, rows)
    for c in range(3):
        low_ref[c] = geom[c][:LY]
        high_ref[c] = geom[c][rows - LY :]
        low_ref[4 + c] = vector[c][:LY]
        high_ref[4 + c] = vector[c][rows - LY :]
        low_ref[7 + c] = push[c][:LY]
        high_ref[7 + c] = push[c][rows - LY :]
    low_ref[3] = geom[3][:LY]
    high_ref[3] = geom[3][rows - LY :]
    high_ref[10] = own_ref[4, rows - LY :, :]
    high_ref[11, : LY // 2, :] = own_ref[5, rows - LY // 2 :, :]
    high_ref[11, LY // 2 :, :] = own_ref[6, rows - LY // 2 :, :]


def coordinates(rows):
    shape = (rows, LZ)
    return (
        lax.broadcasted_iota(jnp.int32, shape, 0),
        lax.broadcasted_iota(jnp.int32, shape, 1),
    )


def up_row(x):
    return pltpu.roll(x, x.shape[0] - 1, 0)


def down_row(x):
    return pltpu.roll(x, 1, 0)


def next_lane(x, x_up, lane):
    return pltpu.roll(jnp.where(lane == 0, x_up, x), LZ - 1, 1)


def bond(mask, delta, contact, allowed=None):
    squared = delta[0] * delta[0] + delta[1] * delta[1] + delta[2] * delta[2]
    live = mask > 0.5
    if allowed is not None:
        live = live & allowed
    squared = jnp.where(live, squared, f32(1.0))
    inverse = 1.0 / (contact * jnp.sqrt(squared))
    tension = (squared * inverse - 1.0) * inverse
    over = inverse * contact
    weight = jnp.sqrt(inverse) * over
    tension = jnp.where(live, tension, f32(0.0))
    weight = jnp.where(live, weight, f32(0.0))
    return tension, [d * weight for d in delta]


def all_bonds(geom, masks, lane, allowed=(None, None, None)):
    total = geom[0].shape[0]
    ahead = [g[LY:] for g in geom]
    base = [g[: total - LY] for g in geom]
    ups = [up_row(g) for g in geom]
    nexts = [next_lane(g, u, lane) for g, u in zip(geom, ups)]

    def build(mask, there, here, ok):
        delta = [a - b for a, b in zip(there[:3], here[:3])]
        return bond(mask, delta, there[3] + here[3], ok)

    return (
        build(masks[0][: total - LY], ahead, base, allowed[0]),
        build(masks[1], ups, geom, allowed[1]),
        build(masks[2], nexts, geom, allowed[2]),
    )


def flux(pair, here, there):
    tension, w = pair
    rel = [a - b for a, b in zip(here, there)]
    along = w[0] * rel[0] + w[1] * rel[1] + w[2] * rel[2]
    return [tension * r + along * n for r, n in zip(rel, w)]


def cut(values, lo, hi):
    return [v[lo:hi] for v in values]


def cut_pair(pair, lo, hi):
    return pair[0][lo:hi], cut(pair[1], lo, hi)


def side_flux(bonds, mid, up, lane, lo, hi):
    fy = flux(cut_pair(bonds[1], lo, hi), mid, up)
    nxt = [next_lane(x, u, lane) for x, u in zip(mid, up)]
    fz = flux(cut_pair(bonds[2], lo, hi), mid, nxt)
    first = lane == 0
    result = []
    for y, z in zip(fy, fz):
        rolled = pltpu.roll(z, 1, 1)
        back = down_row(y + jnp.where(first, rolled, f32(0.0)))
        result.append(y + z - back - jnp.where(first, f32(0.0), rolled))
    return result


def fluxes(bonds, v, lane, lo, hi):
    n = hi - lo
    fx = flux(cut_pair(bonds[0], lo, hi - LY), cut(v, 0, n - LY), cut(v, LY, n))
    side = side_flux(bonds, v, [up_row(x) for x in v], lane[:n], lo, hi)
    result = []
    for s, x in zip(side, fx):
        parts = [x[:LY], -x[n - 2 * LY :]]
        if n > 2 * LY:
            parts.insert(1, x[LY:] - x[: n - 2 * LY])
        result.append(s + jnp.concatenate(parts, axis=0))
    return result


def krylov_kernel(
    odd_ref, ll_ref, far_ref, own_ref, mate_ref, rr_ref, basis_ref, sums_ref
):
    rows = own_ref.shape[1]
    odd = odd_ref[0] == 1
    depth = rows + LY
    total = rows + 2 * depth
    row, lane = coordinates(total)
    half = LY // 2

    def ext(c, low, high):
        outer, mate = far_ref[c], mate_ref[c]
        left = jnp.where(odd, mate, outer)
        right = jnp.where(odd, outer, mate)
        return jnp.concatenate([low, left, own_ref[c], right, high], axis=0)

    none = jnp.zeros((LY, LZ), f32)
    pad = jnp.zeros((LY - half, LZ), f32)
    rim = row == LY - 1
    past = row >= LY
    geom = [ext(c, ll_ref[c], rr_ref[c]) for c in range(4)]
    vector = [ext(7 + c, ll_ref[4 + c], rr_ref[4 + c]) for c in range(3)]
    masks = [
        ext(4, ll_ref[10], none),
        ext(5, jnp.concatenate([pad, ll_ref[11, :half, :]], axis=0), none),
        ext(6, jnp.concatenate([pad, ll_ref[11, half:, :]], axis=0), none),
    ]
    bonds = all_bonds(
        geom, masks, lane, (None, past | rim, past | (rim & (lane == LZ - 1)))
    )

    def operate(v, lo, hi):
        n = hi - lo
        m = n - 2 * LY
        fx = flux(cut_pair(bonds[0], lo, hi - LY), cut(v, 0, n - LY), cut(v, LY, n))
        up = [up_row(x)[8 : n - 8] for x in v]
        side = side_flux(bonds, cut(v, 8, n - 8), up, lane[: n - 16], lo + 8, hi - 8)
        return [
            f32(DIAGONAL_SHIFT) * v[c][LY : LY + m]
            + (fx[c][LY : LY + m] - fx[c][:m])
            + side[c][8 : 8 + m]
            for c in range(3)
        ]

    kept = [cut(vector, depth, depth + rows)]
    push = fluxes(bonds, vector, lane, 0, total)
    lo, hi = 0, total
    before, now = vector, []
    for c in range(3):
        given = jnp.concatenate(
            [ll_ref[7 + c], jnp.zeros((total - 2 * LY, LZ), f32), rr_ref[7 + c]], axis=0
        )
        image = f32(DIAGONAL_SHIFT - CENTER) * vector[c] + push[c] + given
        now.append(image * f32(1.0 / RADIUS))
    kept.append(cut(now, depth, depth + rows))
    for _ in range(1, ITERS):
        image = operate(now, lo, hi)
        m = hi - lo - 2 * LY
        after = [
            (x - f32(CENTER) * y[LY : LY + m]) * f32(2.0 / RADIUS) - p
            for x, y, p in zip(image, now, cut(before, LY, LY + m))
        ]
        before, now = cut(now, LY, LY + m), after
        lo, hi = lo + LY, hi - LY
        kept.append(cut(now, depth - lo, depth - lo + rows))
    for k in range(ITERS + 1):
        for c in range(3):
            basis_ref[3 * k + c] = kept[k][c]

    sub = lax.broadcasted_iota(jnp.int32, (8, LZ), 0)
    col = lax.broadcasted_iota(jnp.int32, (8, LZ), 1)
    line = jnp.zeros((8, LZ), f32)
    for k in range(MOMENTS):
        i = k // 2
        j = k - i
        prod = (
            kept[i][0] * kept[j][0] + kept[i][1] * kept[j][1] + kept[i][2] * kept[j][2]
        )
        part = prod[:8]
        for r in range(8, rows, 8):
            part = part + prod[r : r + 8]
        for s in (4, 2, 1):
            part = part + pltpu.roll(part, s, 0)
        line = jnp.where(sub == k, part, line)
    for s in (64, 32, 16):
        line = line + pltpu.roll(line, s, 1)
    line = jnp.where(col // 16 == sub, line, f32(0.0))
    for s in (4, 2, 1):
        line = line + pltpu.roll(line, s, 0)
    sums_ref[...] = line[:1]


def coefficients(products):
    m = list(products[:2])
    for k in range(2, MOMENTS):
        m.append(2.0 * products[k] - m[k % 2])
    zero = jnp.zeros_like(m[0])
    one = jnp.ones_like(m[0])
    s_before, s = [zero] * MOMENTS, m
    alpha, beta = s[1] / s[0], None
    ratio = alpha
    c_before, c = [zero] * (ITERS + 1), [one] + [zero] * ITERS
    p_before, p = zero, one
    floor = s[0] * f32(1e-12)
    for k in range(ITERS):
        alpha = jnp.clip(alpha, LOWEST, HIGHEST)
        nc = [zero] * (ITERS + 1)
        for l in range(k + 1):
            if l == 0:
                nc[1] = nc[1] + c[0]
            else:
                nc[l - 1] = nc[l - 1] + 0.5 * c[l]
                nc[l + 1] = nc[l + 1] + 0.5 * c[l]
        for l in range(k + 1):
            nc[l] = nc[l] - alpha * c[l]
            if beta is not None and l < k:
                nc[l] = nc[l] - beta * c_before[l]
        np_ = (ORIGIN - alpha) * p
        if beta is not None:
            np_ = np_ - beta * p_before
        if k + 1 < ITERS:
            ns = [zero] * MOMENTS
            for l in range(k + 1, MOMENTS - k - 1):
                ns[l] = 0.5 * (s[l + 1] + s[abs(l - 1)]) - alpha * s[l]
                if beta is not None:
                    ns[l] = ns[l] - beta * s_before[l]
            q = k + 1
            den = jnp.maximum(ns[q], floor)
            factor = 1.0 if q == 1 else 0.5
            next_beta = factor * den / jnp.maximum(s[q - 1], floor)
            new_ratio = ns[q + 1] / den * 0.5
            alpha = new_ratio - ratio
            ratio = new_ratio
            s_before, s = s, ns
            beta = next_beta
        c_before, c = c, nc
        p_before, p = p, np_
    scale = 1.0 / p
    res = [x * scale for x in c]
    sol = []
    for i in range(ITERS):
        total = zero
        for j in range(i + 1, ITERS + 1):
            total = total + res[j] * f32(second_kind(j - 1 - i))
        sol.append(total * f32((-1.0 if i == 0 else -2.0) / RADIUS))
    return res, sol


def finish_kernel(basis_ref, sums_ref, sol_ref, res_ref):
    line = jnp.sum(sums_ref[...], axis=0)
    line = jnp.sum(line, axis=0, keepdims=True)
    line = jnp.broadcast_to(line, (8, LZ))
    for s in (8, 4, 2, 1):
        line = line + pltpu.roll(line, s, 1)
    products = [
        jnp.broadcast_to(line[:, 16 * k + 15 : 16 * k + 16], (8, LZ))
        for k in range(MOMENTS)
    ]
    res, sol = coefficients(products)
    rows = basis_ref.shape[1]
    for c in range(3):
        for r in range(0, rows, 8):
            t = [basis_ref[3 * k + c, r : r + 8, :] for k in range(ITERS + 1)]
            x = sol[0] * t[0]
            for k in range(1, ITERS):
                x = x + sol[k] * t[k]
            y = res[0] * t[0]
            for k in range(1, ITERS + 1):
                y = y + res[k] * t[k]
            sol_ref[r : r + 8, c, :] = x
            res_ref[r : r + 8, c, :] = y


def by_rows(array):
    return array.reshape(array.shape[0], -1, LZ).transpose(1, 0, 2)


def stay(array):
    return pltpu.with_memory_space_constraint(array, pltpu.HBM)


def on_device(positions, radii, neighbours, right_side):
    owned = positions.shape[1]
    rows = owned // LZ
    devices = lax.axis_size("gx")
    place = lax.axis_index("gx").astype(jnp.int32)
    first = (place * owned).reshape(1)
    odd = (place % 2).reshape(1)
    vmem = pl.BlockSpec(memory_space=pltpu.VMEM)
    smem = pl.BlockSpec(memory_space=pltpu.SMEM)
    hbm = pl.BlockSpec(memory_space=pltpu.HBM)

    packed = pl.pallas_call(
        pack_kernel,
        out_shape=jax.ShapeDtypeStruct((10, rows, LZ), f32),
        in_specs=[smem, hbm, hbm, hbm, hbm],
        out_specs=vmem,
        scratch_shapes=[
            pltpu.VMEM((rows, 3, LZ), f32),
            pltpu.VMEM((rows, LZ), f32),
            pltpu.VMEM((rows, neighbours.shape[0], LZ), jnp.int32),
            pltpu.VMEM((rows, 3, LZ), f32),
            pltpu.SemaphoreType.DMA((4,)),
        ],
        compiler_params=pltpu.CompilerParams(vmem_limit_bytes=4 << 20),
        name="pack",
    )(
        first,
        stay(by_rows(positions)),
        stay(radii.reshape(rows, LZ)),
        stay(by_rows(neighbours)),
        stay(by_rows(right_side)),
    )

    def moved(array, to):
        return lax.ppermute(array, "gx", [(i, to(i) % devices) for i in range(devices)])

    low, high = pl.pallas_call(
        edge_kernel,
        out_shape=(
            jax.ShapeDtypeStruct((10, LY, LZ), f32),
            jax.ShapeDtypeStruct((12, LY, LZ), f32),
        ),
        in_specs=[vmem],
        out_specs=(vmem, vmem),
        compiler_params=pltpu.CompilerParams(vmem_limit_bytes=4 << 20),
        name="edge",
    )(packed)
    across = moved(packed, lambda i: i + 1 if i % 2 else i - 1)
    far_left = moved(high, lambda i: i + 2)
    far_right = moved(low, lambda i: i - 2)
    mate = moved(packed, lambda i: i ^ 1)

    basis, sums = pl.pallas_call(
        krylov_kernel,
        out_shape=(
            jax.ShapeDtypeStruct((3 * (ITERS + 1), rows, LZ), f32),
            jax.ShapeDtypeStruct((1, LZ), f32),
        ),
        in_specs=[smem] + [vmem] * 5,
        out_specs=(vmem, vmem),
        compiler_params=pltpu.CompilerParams(vmem_limit_bytes=12 << 20),
        name="krylov",
    )(odd, far_left, across, packed, mate, far_right)

    chips = devices // 2
    sums = sums + moved(sums, lambda i: i ^ 1)
    groups = [[2 * ((z + chips // 2) % chips) + c for z in range(chips)] for c in (0, 1)]
    everyone = lax.all_to_all(
        jnp.broadcast_to(sums[None], (chips, 1, LZ)),
        "gx",
        split_axis=0,
        concat_axis=0,
        tiled=True,
        axis_index_groups=groups,
    )

    sol, res = pl.pallas_call(
        finish_kernel,
        out_shape=(
            jax.ShapeDtypeStruct((rows, 3, LZ), f32),
            jax.ShapeDtypeStruct((rows, 3, LZ), f32),
        ),
        in_specs=[vmem, vmem],
        out_specs=(vmem, vmem),
        compiler_params=pltpu.CompilerParams(vmem_limit_bytes=4 << 20),
        name="finish",
    )(basis, everyone.reshape(-1, 8, LZ))
    back = lambda a: a.transpose(1, 0, 2).reshape(3, owned)
    return back(sol), back(res)


def solution(mesh):
    return jax.shard_map(
        on_device,
        mesh=mesh,
        in_specs=(
            P(None, ("groups", "gx")),
            P(("groups", "gx")),
            P(None, ("groups", "gx")),
            P(None, ("groups", "gx")),
        ),
        out_specs=(P(None, ("groups", "gx")), P(None, ("groups", "gx"))),
        check_vma=False,
    )
```

```python
import jax
import jax.numpy as jnp
from jax import lax
from jax.experimental import pallas as pl
from jax.experimental.pallas import tpu as pltpu
from jax.sharding import PartitionSpec as P


LY = 16
LZ = 128
ITERS = 4
DIAGONAL_SHIFT = 4.0

CENTER = 5.7
RADIUS = 2.3
ORIGIN = -CENTER / RADIUS
MOMENTS = 2 * ITERS
LOWEST, HIGHEST = -2.2, 4.6

f32 = jnp.float32


def second_kind(order):
    below, value = 0.0, 1.0
    for _ in range(order):
        below, value = value, 2.0 * ORIGIN * value - below
    return value


def pack_kernel(first_ref, pos_hbm, rad_hbm, nb_hbm, rhs_hbm, out_ref, *scratch):
    pos_ref, rad_ref, nb_ref, rhs_ref, sems = scratch
    moves = [
        pltpu.make_async_copy(src, dst, sems.at[k])
        for k, (src, dst) in enumerate(
            (
                (nb_hbm, nb_ref),
                (pos_hbm, pos_ref),
                (rhs_hbm, rhs_ref),
                (rad_hbm, rad_ref),
            )
        )
    ]
    for move in moves:
        move.start()
    rows = rad_ref.shape[0]
    shape = (rows, LZ)
    ids = first_ref[0] + (
        lax.broadcasted_iota(jnp.int32, shape, 0) * LZ
        + lax.broadcasted_iota(jnp.int32, shape, 1)
    )
    for move in moves:
        move.wait()
    slots = [nb_ref[:, s, :] - ids for s in range(nb_ref.shape[1])]
    for b, shift in enumerate((LY * LZ, LZ, 1)):
        hit = slots[0] == shift
        for other in slots[1:]:
            hit = hit | (other == shift)
        out_ref[4 + b] = jnp.where(hit, f32(1.0), f32(0.0))
    for c in range(3):
        out_ref[c] = pos_ref[:, c, :]
        out_ref[7 + c] = rhs_ref[:, c, :]
    out_ref[3] = rad_ref[...]


def edge_kernel(own_ref, low_ref, high_ref):
    rows = own_ref.shape[1]
    row, lane = coordinates(rows)
    geom = [own_ref[c] for c in range(4)]
    inside = row < rows - 1
    last = (row == rows - 1) & (lane == LZ - 1)
    vector = [own_ref[7 + c] for c in range(3)]
    bonds = all_bonds(
        geom,
        [own_ref[4], own_ref[5], own_ref[6]],
        lane,
        (None, inside, jnp.logical_not(last)),
    )
    push = fluxes(bonds, vector, lane, 0, rows)
    for c in range(3):
        low_ref[c] = geom[c][:LY]
        high_ref[c] = geom[c][rows - LY :]
        low_ref[4 + c] = vector[c][:LY]
        high_ref[4 + c] = vector[c][rows - LY :]
        low_ref[7 + c] = push[c][:LY]
        high_ref[7 + c] = push[c][rows - LY :]
    low_ref[3] = geom[3][:LY]
    high_ref[3] = geom[3][rows - LY :]
    high_ref[10] = own_ref[4, rows - LY :, :]
    high_ref[11, : LY // 2, :] = own_ref[5, rows - LY // 2 :, :]
    high_ref[11, LY // 2 :, :] = own_ref[6, rows - LY // 2 :, :]


def coordinates(rows):
    shape = (rows, LZ)
    return (
        lax.broadcasted_iota(jnp.int32, shape, 0),
        lax.broadcasted_iota(jnp.int32, shape, 1),
    )


def up_row(x):
    return pltpu.roll(x, x.shape[0] - 1, 0)


def down_row(x):
    return pltpu.roll(x, 1, 0)


def next_lane(x, x_up, lane):
    return pltpu.roll(jnp.where(lane == 0, x_up, x), LZ - 1, 1)


def bond(mask, delta, contact, allowed=None):
    squared = delta[0] * delta[0] + delta[1] * delta[1] + delta[2] * delta[2]
    live = mask > 0.5
    if allowed is not None:
        live = live & allowed
    squared = jnp.where(live, squared, f32(1.0))
    shrink = lax.rsqrt(squared)
    inverse = 1.0 / (contact * (squared * shrink))
    scaled = inverse * f32(2.0 / RADIUS)
    tension = (squared * inverse - 1.0) * scaled
    weight = (scaled * lax.rsqrt(scaled)) * shrink
    tension = jnp.where(live, tension, f32(0.0))
    weight = jnp.where(live, weight, f32(0.0))
    return tension, [d * weight for d in delta]


def all_bonds(geom, masks, lane, allowed=(None, None, None)):
    total = geom[0].shape[0]
    ahead = [g[LY:] for g in geom]
    base = [g[: total - LY] for g in geom]
    ups = [up_row(g) for g in geom]
    nexts = [next_lane(g, u, lane) for g, u in zip(geom, ups)]

    def build(mask, there, here, ok):
        delta = [a - b for a, b in zip(there[:3], here[:3])]
        return bond(mask, delta, there[3] + here[3], ok)

    return (
        build(masks[0][: total - LY], ahead, base, allowed[0]),
        build(masks[1], ups, geom, allowed[1]),
        build(masks[2], nexts, geom, allowed[2]),
    )


def flux(pair, here, there):
    tension, w = pair
    rel = [a - b for a, b in zip(here, there)]
    along = w[0] * rel[0] + w[1] * rel[1] + w[2] * rel[2]
    return [tension * r + along * n for r, n in zip(rel, w)]


def cut(values, lo, hi):
    return [v[lo:hi] for v in values]


def cut_pair(pair, lo, hi):
    return pair[0][lo:hi], cut(pair[1], lo, hi)


def side_flux(bonds, mid, up, lane, lo, hi):
    fy = flux(cut_pair(bonds[1], lo, hi), mid, up)
    nxt = [next_lane(x, u, lane) for x, u in zip(mid, up)]
    fz = flux(cut_pair(bonds[2], lo, hi), mid, nxt)
    first = lane == 0
    result = []
    for y, z in zip(fy, fz):
        rolled = pltpu.roll(z, 1, 1)
        back = down_row(y + jnp.where(first, rolled, f32(0.0)))
        result.append(y + z - back - jnp.where(first, f32(0.0), rolled))
    return result


def fluxes(bonds, v, lane, lo, hi):
    n = hi - lo
    fx = flux(cut_pair(bonds[0], lo, hi - LY), cut(v, 0, n - LY), cut(v, LY, n))
    side = side_flux(bonds, v, [up_row(x) for x in v], lane[:n], lo, hi)
    result = []
    for s, x in zip(side, fx):
        parts = [x[:LY], -x[n - 2 * LY :]]
        if n > 2 * LY:
            parts.insert(1, x[LY:] - x[: n - 2 * LY])
        result.append(s + jnp.concatenate(parts, axis=0))
    return result


def krylov_kernel(
    odd_ref, ll_ref, far_ref, own_ref, mate_ref, rr_ref, basis_ref, sums_ref
):
    rows = own_ref.shape[1]
    odd = odd_ref[0] == 1
    depth = rows + LY
    total = rows + 2 * depth
    row, lane = coordinates(total)
    half = LY // 2

    def ext(c, low, high):
        outer, mate = far_ref[c], mate_ref[c]
        left = jnp.where(odd, mate, outer)
        right = jnp.where(odd, outer, mate)
        return jnp.concatenate([low, left, own_ref[c], right, high], axis=0)

    none = jnp.zeros((LY, LZ), f32)
    pad = jnp.zeros((LY - half, LZ), f32)
    rim = row == LY - 1
    past = row >= LY
    geom = [ext(c, ll_ref[c], rr_ref[c]) for c in range(4)]
    vector = [ext(7 + c, ll_ref[4 + c], rr_ref[4 + c]) for c in range(3)]
    masks = [
        ext(4, ll_ref[10], none),
        ext(5, jnp.concatenate([pad, ll_ref[11, :half, :]], axis=0), none),
        ext(6, jnp.concatenate([pad, ll_ref[11, half:, :]], axis=0), none),
    ]
    bonds = all_bonds(
        geom, masks, lane, (None, past | rim, past | (rim & (lane == LZ - 1)))
    )

    def operate(v, lo, hi):
        n = hi - lo
        m = n - 2 * LY
        fx = flux(cut_pair(bonds[0], lo, hi - LY), cut(v, 0, n - LY), cut(v, LY, n))
        up = [up_row(x[8 : n - 8])[: n - 24] for x in v]
        mid = cut(v, 8, n - LY)
        side = side_flux(bonds, mid, up, lane[: n - 24], lo + 8, hi - LY)
        return [
            f32(2.0 * (DIAGONAL_SHIFT - CENTER) / RADIUS) * v[c][LY : LY + m]
            + (fx[c][LY : LY + m] - fx[c][:m])
            + side[c][8 : 8 + m]
            for c in range(3)
        ]

    kept = [cut(vector, depth, depth + rows)]
    push = fluxes(bonds, vector, lane, 0, total)
    lo, hi = 0, total
    before, now = vector, []
    for c in range(3):
        given = jnp.concatenate(
            [ll_ref[7 + c], jnp.zeros((total - 2 * LY, LZ), f32), rr_ref[7 + c]], axis=0
        )
        image = f32(2.0 * (DIAGONAL_SHIFT - CENTER) / RADIUS) * vector[c]
        now.append(f32(0.5) * (image + push[c] + given))
    kept.append(cut(now, depth, depth + rows))
    for _ in range(1, ITERS):
        image = operate(now, lo, hi)
        m = hi - lo - 2 * LY
        after = [x - p for x, p in zip(image, cut(before, LY, LY + m))]
        before, now = cut(now, LY, LY + m), after
        lo, hi = lo + LY, hi - LY
        kept.append(cut(now, depth - lo, depth - lo + rows))
    for k in range(ITERS + 1):
        for c in range(3):
            basis_ref[3 * k + c] = kept[k][c]

    sub = lax.broadcasted_iota(jnp.int32, (8, LZ), 0)
    col = lax.broadcasted_iota(jnp.int32, (8, LZ), 1)
    line = jnp.zeros((8, LZ), f32)
    for k in range(MOMENTS):
        i = k // 2
        j = k - i
        prod = (
            kept[i][0] * kept[j][0] + kept[i][1] * kept[j][1] + kept[i][2] * kept[j][2]
        )
        part = prod[:8]
        for r in range(8, rows, 8):
            part = part + prod[r : r + 8]
        for s in (4, 2, 1):
            part = part + pltpu.roll(part, s, 0)
        line = jnp.where(sub == k, part, line)
    for s in (64, 32, 16):
        line = line + pltpu.roll(line, s, 1)
    line = jnp.where(col // 16 == sub, line, f32(0.0))
    for s in (4, 2, 1):
        line = line + pltpu.roll(line, s, 0)
    sums_ref[...] = line[:1]


def coefficients(products):
    m = list(products[:2])
    for k in range(2, MOMENTS):
        m.append(2.0 * products[k] - m[k % 2])
    zero = jnp.zeros_like(m[0])
    one = jnp.ones_like(m[0])
    s_before, s = [zero] * MOMENTS, m
    alpha, beta = s[1] / s[0], None
    ratio = alpha
    c_before, c = [zero] * (ITERS + 1), [one] + [zero] * ITERS
    p_before, p = zero, one
    floor = s[0] * f32(1e-12)
    for k in range(ITERS):
        alpha = jnp.clip(alpha, LOWEST, HIGHEST)
        nc = [zero] * (ITERS + 1)
        for l in range(k + 1):
            if l == 0:
                nc[1] = nc[1] + c[0]
            else:
                nc[l - 1] = nc[l - 1] + 0.5 * c[l]
                nc[l + 1] = nc[l + 1] + 0.5 * c[l]
        for l in range(k + 1):
            nc[l] = nc[l] - alpha * c[l]
            if beta is not None and l < k:
                nc[l] = nc[l] - beta * c_before[l]
        np_ = (ORIGIN - alpha) * p
        if beta is not None:
            np_ = np_ - beta * p_before
        if k + 1 < ITERS:
            ns = [zero] * MOMENTS
            for l in range(k + 1, MOMENTS - k - 1):
                ns[l] = 0.5 * (s[l + 1] + s[abs(l - 1)]) - alpha * s[l]
                if beta is not None:
                    ns[l] = ns[l] - beta * s_before[l]
            q = k + 1
            den = jnp.maximum(ns[q], floor)
            factor = 1.0 if q == 1 else 0.5
            next_beta = factor * den / jnp.maximum(s[q - 1], floor)
            new_ratio = ns[q + 1] / den * 0.5
            alpha = new_ratio - ratio
            ratio = new_ratio
            s_before, s = s, ns
            beta = next_beta
        c_before, c = c, nc
        p_before, p = p, np_
    scale = 1.0 / p
    res = [x * scale for x in c]
    sol = []
    for i in range(ITERS):
        total = zero
        for j in range(i + 1, ITERS + 1):
            total = total + res[j] * f32(second_kind(j - 1 - i))
        sol.append(total * f32((-1.0 if i == 0 else -2.0) / RADIUS))
    return res, sol


def finish_kernel(
    basis_ref, sums_ref, sol_hbm, res_hbm, sol_ref, res_ref, sems
):
    line = jnp.sum(sums_ref[...], axis=0)
    line = jnp.sum(line, axis=0, keepdims=True)
    line = jnp.broadcast_to(line, (8, LZ))
    for s in (8, 4, 2, 1):
        line = line + pltpu.roll(line, s, 1)
    products = [
        jnp.broadcast_to(line[:, 16 * k + 15 : 16 * k + 16], (8, LZ))
        for k in range(MOMENTS)
    ]
    res, sol = coefficients(products)
    rows = basis_ref.shape[1]

    def combine(weights, to_ref):
        for c in range(3):
            for r in range(0, rows, 8):
                x = weights[0] * basis_ref[c, r : r + 8, :]
                for k in range(1, len(weights)):
                    x = x + weights[k] * basis_ref[3 * k + c, r : r + 8, :]
                to_ref[r : r + 8, c, :] = x

    leave = [
        pltpu.make_async_copy(sol_ref, sol_hbm, sems.at[0]),
        pltpu.make_async_copy(res_ref, res_hbm, sems.at[1]),
    ]
    combine(res, res_ref)
    leave[1].start()
    combine(sol, sol_ref)
    leave[0].start()
    leave[1].wait()
    leave[0].wait()


def by_rows(array):
    return array.reshape(array.shape[0], -1, LZ).transpose(1, 0, 2)


def stay(array):
    return pltpu.with_memory_space_constraint(array, pltpu.HBM)


def on_device(positions, radii, neighbours, right_side):
    owned = positions.shape[1]
    rows = owned // LZ
    devices = lax.axis_size("gx")
    place = lax.axis_index("gx").astype(jnp.int32)
    first = (place * owned).reshape(1)
    odd = (place % 2).reshape(1)
    vmem = pl.BlockSpec(memory_space=pltpu.VMEM)
    smem = pl.BlockSpec(memory_space=pltpu.SMEM)
    hbm = pl.BlockSpec(memory_space=pltpu.HBM)

    packed = pl.pallas_call(
        pack_kernel,
        out_shape=jax.ShapeDtypeStruct((10, rows, LZ), f32),
        in_specs=[smem, hbm, hbm, hbm, hbm],
        out_specs=vmem,
        scratch_shapes=[
            pltpu.VMEM((rows, 3, LZ), f32),
            pltpu.VMEM((rows, LZ), f32),
            pltpu.VMEM((rows, neighbours.shape[0], LZ), jnp.int32),
            pltpu.VMEM((rows, 3, LZ), f32),
            pltpu.SemaphoreType.DMA((4,)),
        ],
        compiler_params=pltpu.CompilerParams(vmem_limit_bytes=4 << 20),
        name="pack",
    )(
        first,
        stay(by_rows(positions)),
        stay(radii.reshape(rows, LZ)),
        stay(by_rows(neighbours)),
        stay(by_rows(right_side)),
    )

    def moved(array, to):
        return lax.ppermute(array, "gx", [(i, to(i) % devices) for i in range(devices)])

    low, high = pl.pallas_call(
        edge_kernel,
        out_shape=(
            jax.ShapeDtypeStruct((10, LY, LZ), f32),
            jax.ShapeDtypeStruct((12, LY, LZ), f32),
        ),
        in_specs=[vmem],
        out_specs=(vmem, vmem),
        compiler_params=pltpu.CompilerParams(vmem_limit_bytes=4 << 20),
        name="edge",
    )(packed)
    across = moved(packed, lambda i: i + 1 if i % 2 else i - 1)
    far_left = moved(high, lambda i: i + 2)
    far_right = moved(low, lambda i: i - 2)
    mate = moved(packed, lambda i: i ^ 1)

    basis, sums = pl.pallas_call(
        krylov_kernel,
        out_shape=(
            jax.ShapeDtypeStruct((3 * (ITERS + 1), rows, LZ), f32),
            jax.ShapeDtypeStruct((1, LZ), f32),
        ),
        in_specs=[smem] + [vmem] * 5,
        out_specs=(vmem, vmem),
        compiler_params=pltpu.CompilerParams(vmem_limit_bytes=12 << 20),
        name="krylov",
    )(odd, far_left, across, packed, mate, far_right)

    chips = devices // 2
    sums = sums + moved(sums, lambda i: i ^ 1)
    groups = [[2 * ((z + chips // 2) % chips) + c for z in range(chips)] for c in (0, 1)]
    everyone = lax.all_to_all(
        jnp.broadcast_to(sums[None], (chips, 1, LZ)),
        "gx",
        split_axis=0,
        concat_axis=0,
        tiled=True,
        axis_index_groups=groups,
    )

    sol, res = pl.pallas_call(
        finish_kernel,
        out_shape=(
            jax.ShapeDtypeStruct((rows, 3, LZ), f32),
            jax.ShapeDtypeStruct((rows, 3, LZ), f32),
        ),
        in_specs=[vmem, vmem],
        out_specs=(hbm, hbm),
        scratch_shapes=[
            pltpu.VMEM((rows, 3, LZ), f32),
            pltpu.VMEM((rows, 3, LZ), f32),
            pltpu.SemaphoreType.DMA((2,)),
        ],
        compiler_params=pltpu.CompilerParams(vmem_limit_bytes=4 << 20),
        name="finish",
    )(basis, everyone.reshape(-1, 8, LZ))
    back = lambda a: a.transpose(1, 0, 2).reshape(3, owned)
    return back(sol), back(res)


def solution(mesh):
    return jax.shard_map(
        on_device,
        mesh=mesh,
        in_specs=(
            P(None, ("groups", "gx")),
            P(("groups", "gx")),
            P(None, ("groups", "gx")),
            P(None, ("groups", "gx")),
        ),
        out_specs=(P(None, ("groups", "gx")), P(None, ("groups", "gx"))),
        check_vma=False,
    )
```

```python
import jax
import jax.numpy as jnp
from jax import lax
from jax.experimental import pallas as pl
from jax.experimental.pallas import tpu as pltpu
from jax.sharding import PartitionSpec as P


LY = 16
LZ = 128
ITERS = 4
DIAGONAL_SHIFT = 4.0

CENTER = 5.7
RADIUS = 2.3
STILL = (DIAGONAL_SHIFT - CENTER) / RADIUS
ORIGIN = -CENTER / RADIUS
MOMENTS = 2 * ITERS

f32 = jnp.float32


def first_kind(order, at):
    below, value = at, 1.0
    for _ in range(order):
        below, value = value, 2.0 * at * value - below
    return value


def quotient(order, at):
    second = [1.0, 2.0 * at]
    while len(second) < order:
        second.append(2.0 * at * second[-1] - second[-2])
    return [(1.0 if i == 0 else 2.0) * second[order - 1 - i] for i in range(order)]


def pack_kernel(first_ref, pos_hbm, rad_hbm, nb_hbm, rhs_hbm, out_ref, *scratch):
    pos_ref, rad_ref, nb_ref, rhs_ref, sems = scratch
    moves = [
        pltpu.make_async_copy(src, dst, sems.at[k])
        for k, (src, dst) in enumerate(
            (
                (nb_hbm, nb_ref),
                (pos_hbm, pos_ref),
                (rhs_hbm, rhs_ref),
                (rad_hbm, rad_ref),
            )
        )
    ]
    for move in moves:
        move.start()
    rows = rad_ref.shape[0]
    shape = (rows, LZ)
    ids = first_ref[0] + (
        lax.broadcasted_iota(jnp.int32, shape, 0) * LZ
        + lax.broadcasted_iota(jnp.int32, shape, 1)
    )
    for move in moves:
        move.wait()
    slots = [nb_ref[:, s, :] - ids for s in range(nb_ref.shape[1])]
    for b, shift in enumerate((LY * LZ, LZ, 1)):
        hit = slots[0] == shift
        for other in slots[1:]:
            hit = hit | (other == shift)
        out_ref[4 + b] = jnp.where(hit, f32(1.0), f32(0.0))
    for c in range(3):
        out_ref[c] = pos_ref[:, c, :]
        out_ref[7 + c] = rhs_ref[:, c, :]
    out_ref[3] = rad_ref[...]


def edge_kernel(own_ref, low_ref, high_ref):
    rows = own_ref.shape[1]
    row, lane = coordinates(rows)
    geom = [own_ref[c] for c in range(4)]
    inside = row < rows - 1
    last = (row == rows - 1) & (lane == LZ - 1)
    vector = [own_ref[7 + c] for c in range(3)]
    bonds = all_bonds(
        geom,
        [own_ref[4], own_ref[5], own_ref[6]],
        lane,
        (None, inside, jnp.logical_not(last)),
    )
    push = fluxes(bonds, vector, lane, 0, rows)
    for c in range(3):
        low_ref[c] = geom[c][:LY]
        high_ref[c] = geom[c][rows - LY :]
        low_ref[4 + c] = vector[c][:LY]
        high_ref[4 + c] = vector[c][rows - LY :]
        low_ref[7 + c] = push[c][:LY]
        high_ref[7 + c] = push[c][rows - LY :]
    low_ref[3] = geom[3][:LY]
    high_ref[3] = geom[3][rows - LY :]
    high_ref[10] = own_ref[4, rows - LY :, :]
    high_ref[11, : LY // 2, :] = own_ref[5, rows - LY // 2 :, :]
    high_ref[11, LY // 2 :, :] = own_ref[6, rows - LY // 2 :, :]


def coordinates(rows):
    shape = (rows, LZ)
    return (
        lax.broadcasted_iota(jnp.int32, shape, 0),
        lax.broadcasted_iota(jnp.int32, shape, 1),
    )


def up_row(x):
    return pltpu.roll(x, x.shape[0] - 1, 0)


def down_row(x):
    return pltpu.roll(x, 1, 0)


def next_lane(x, x_up, lane):
    return pltpu.roll(jnp.where(lane == 0, x_up, x), LZ - 1, 1)


def bond(mask, delta, contact, allowed=None):
    squared = delta[0] * delta[0] + delta[1] * delta[1] + delta[2] * delta[2]
    live = mask > 0.5
    if allowed is not None:
        live = live & allowed
    squared = jnp.where(live, squared, f32(1.0))
    shrink = lax.rsqrt(squared)
    inverse = 1.0 / (contact * (squared * shrink))
    scaled = inverse * f32(2.0 / RADIUS)
    tension = (squared * inverse - 1.0) * scaled
    weight = (scaled * lax.rsqrt(scaled)) * shrink
    tension = jnp.where(live, tension, f32(0.0))
    weight = jnp.where(live, weight, f32(0.0))
    return tension, [d * weight for d in delta]


def all_bonds(geom, masks, lane, allowed=(None, None, None)):
    total = geom[0].shape[0]
    ahead = [g[LY:] for g in geom]
    base = [g[: total - LY] for g in geom]
    ups = [up_row(g) for g in geom]
    nexts = [next_lane(g, u, lane) for g, u in zip(geom, ups)]

    def build(mask, there, here, ok):
        delta = [a - b for a, b in zip(there[:3], here[:3])]
        return bond(mask, delta, there[3] + here[3], ok)

    return (
        build(masks[0][: total - LY], ahead, base, allowed[0]),
        build(masks[1], ups, geom, allowed[1]),
        build(masks[2], nexts, geom, allowed[2]),
    )


def flux(pair, here, there):
    tension, w = pair
    rel = [a - b for a, b in zip(here, there)]
    along = w[0] * rel[0] + w[1] * rel[1] + w[2] * rel[2]
    return [tension * r + along * n for r, n in zip(rel, w)]


def cut(values, lo, hi):
    return [v[lo:hi] for v in values]


def cut_pair(pair, lo, hi):
    return pair[0][lo:hi], cut(pair[1], lo, hi)


def side_flux(bonds, mid, up, lane, lo, hi):
    fy = flux(cut_pair(bonds[1], lo, hi), mid, up)
    nxt = [next_lane(x, u, lane) for x, u in zip(mid, up)]
    fz = flux(cut_pair(bonds[2], lo, hi), mid, nxt)
    first = lane == 0
    result = []
    for y, z in zip(fy, fz):
        rolled = pltpu.roll(z, 1, 1)
        back = down_row(y + jnp.where(first, rolled, f32(0.0)))
        result.append(y + z - back - jnp.where(first, f32(0.0), rolled))
    return result


def fluxes(bonds, v, lane, lo, hi):
    n = hi - lo
    fx = flux(cut_pair(bonds[0], lo, hi - LY), cut(v, 0, n - LY), cut(v, LY, n))
    side = side_flux(bonds, v, [up_row(x) for x in v], lane[:n], lo, hi)
    result = []
    for s, x in zip(side, fx):
        parts = [x[:LY], -x[n - 2 * LY :]]
        if n > 2 * LY:
            parts.insert(1, x[LY:] - x[: n - 2 * LY])
        result.append(s + jnp.concatenate(parts, axis=0))
    return result


def krylov_kernel(
    odd_ref, ll_ref, far_ref, own_ref, mate_ref, rr_ref, basis_ref, sums_ref
):
    rows = own_ref.shape[1]
    odd = odd_ref[0] == 1
    depth = rows + LY
    total = rows + 2 * depth
    row, lane = coordinates(total)
    half = LY // 2

    def ext(c, low, high):
        outer, mate = far_ref[c], mate_ref[c]
        left = jnp.where(odd, mate, outer)
        right = jnp.where(odd, outer, mate)
        return jnp.concatenate([low, left, own_ref[c], right, high], axis=0)

    none = jnp.zeros((LY, LZ), f32)
    pad = jnp.zeros((LY - half, LZ), f32)
    rim = row == LY - 1
    past = row >= LY
    geom = [ext(c, ll_ref[c], rr_ref[c]) for c in range(4)]
    vector = [ext(7 + c, ll_ref[4 + c], rr_ref[4 + c]) for c in range(3)]
    masks = [
        ext(4, ll_ref[10], none),
        ext(5, jnp.concatenate([pad, ll_ref[11, :half, :]], axis=0), none),
        ext(6, jnp.concatenate([pad, ll_ref[11, half:, :]], axis=0), none),
    ]
    bonds = all_bonds(
        geom, masks, lane, (None, past | rim, past | (rim & (lane == LZ - 1)))
    )

    def operate(v, lo, hi):
        n = hi - lo
        m = n - 2 * LY
        fx = flux(cut_pair(bonds[0], lo, hi - LY), cut(v, 0, n - LY), cut(v, LY, n))
        up = [up_row(x[8 : n - 8])[: n - 24] for x in v]
        mid = cut(v, 8, n - LY)
        side = side_flux(bonds, mid, up, lane[: n - 24], lo + 8, hi - LY)
        return [
            f32(2.0 * (DIAGONAL_SHIFT - CENTER) / RADIUS) * v[c][LY : LY + m]
            + (fx[c][LY : LY + m] - fx[c][:m])
            + side[c][8 : 8 + m]
            for c in range(3)
        ]

    kept = [cut(vector, depth, depth + rows)]
    push = fluxes(bonds, vector, lane, 0, total)
    lo, hi = 0, total
    before, now = None, []
    for c in range(3):
        given = [ll_ref[7 + c], jnp.zeros((total - 2 * LY, LZ), f32), rr_ref[7 + c]]
        now.append(push[c] + jnp.concatenate(given, axis=0))
    kept.append(cut(now, depth, depth + rows))
    for k in range(1, ITERS):
        image = operate(now, lo, hi)
        m = hi - lo - 2 * LY
        if k == 1:
            after = [f32(0.5) * x for x in image]
        else:
            after = [x - p for x, p in zip(image, cut(before, LY, LY + m))]
        before, now = cut(now, LY, LY + m), after
        lo, hi = lo + LY, hi - LY
        kept.append(cut(now, depth - lo, depth - lo + rows))
    for k in range(ITERS + 1):
        for c in range(3):
            basis_ref[3 * k + c] = kept[k][c]

    sub = lax.broadcasted_iota(jnp.int32, (8, LZ), 0)
    col = lax.broadcasted_iota(jnp.int32, (8, LZ), 1)
    line = jnp.zeros((8, LZ), f32)
    for k in range(MOMENTS):
        i = k // 2
        j = k - i
        prod = (
            kept[i][0] * kept[j][0] + kept[i][1] * kept[j][1] + kept[i][2] * kept[j][2]
        )
        part = prod[:8]
        for r in range(8, rows, 8):
            part = part + prod[r : r + 8]
        for s in (4, 2, 1):
            part = part + pltpu.roll(part, s, 0)
        line = jnp.where(sub == k, part, line)
    for s in (64, 32, 16):
        line = line + pltpu.roll(line, s, 1)
    line = jnp.where(col // 16 == sub, line, f32(0.0))
    for s in (4, 2, 1):
        line = line + pltpu.roll(line, s, 0)
    sums_ref[...] = line[:1]


def coefficients(products):
    size = ITERS + 1
    zero = jnp.zeros_like(products[0])
    nu = list(products[2:4])
    for k in range(2, MOMENTS - 2):
        nu.append(2.0 * products[2 + k] - nu[k % 2])
    gram = [[None] * size for _ in range(size)]
    gram[0][0] = products[0]
    for k in range(1, size):
        value = products[1] * f32(first_kind(k - 1, STILL))
        for i, q in enumerate(quotient(k - 1, STILL) if k > 1 else ()):
            value = value + nu[i] * f32(0.5 * q)
        gram[0][k] = value
    for i in range(1, ITERS):
        for j in range(i, size):
            gram[i][j] = 0.5 * (nu[i + j - 2] + nu[j - i])
    scale = [gram[i][i] * f32(1e-8) for i in range(ITERS)]
    lower = [[None] * ITERS for _ in range(size)]
    for i in range(ITERS):
        pivot = gram[i][i]
        inverse = 1.0 / pivot
        if i:
            inverse = jnp.where(pivot > scale[i], inverse, zero)
        for j in range(i + 1, size):
            lower[j][i] = gram[i][j] * inverse
        for k in range(i + 1, ITERS):
            for j in range(k, size):
                gram[k][j] = gram[k][j] - lower[k][i] * gram[i][j]
    res = [None] * ITERS + [zero + 1.0]
    for i in reversed(range(ITERS)):
        value = lower[ITERS][i]
        for j in range(i + 1, ITERS):
            value = value + lower[j][i] * res[j]
        res[i] = -value
    at_origin = res[0]
    for k in range(1, size):
        weight = -2.0 * DIAGONAL_SHIFT / RADIUS * first_kind(k - 1, ORIGIN)
        at_origin = at_origin + res[k] * f32(weight)
    unit = 1.0 / at_origin
    res = [x * unit for x in res]
    sol = [zero] * ITERS
    for j in range(1, size):
        sol[0] = sol[0] - res[j] * f32(2.0 / RADIUS * first_kind(j - 1, ORIGIN))
        for i, q in enumerate(quotient(j - 1, ORIGIN) if j > 1 else ()):
            sol[i + 1] = sol[i + 1] - res[j] * f32(q / RADIUS)
    return res, sol


def finish_kernel(
    basis_ref, sums_ref, sol_hbm, res_hbm, sol_ref, res_ref, sems
):
    line = jnp.sum(sums_ref[...], axis=0)
    line = jnp.sum(line, axis=0, keepdims=True)
    line = jnp.broadcast_to(line, (8, LZ))
    for s in (8, 4, 2, 1):
        line = line + pltpu.roll(line, s, 1)
    products = [
        jnp.broadcast_to(line[:, 16 * k + 15 : 16 * k + 16], (8, LZ))
        for k in range(MOMENTS)
    ]
    res, sol = coefficients(products)
    rows = basis_ref.shape[1]

    def combine(weights, to_ref):
        for c in range(3):
            for r in range(0, rows, 8):
                x = weights[0] * basis_ref[c, r : r + 8, :]
                for k in range(1, len(weights)):
                    x = x + weights[k] * basis_ref[3 * k + c, r : r + 8, :]
                to_ref[r : r + 8, c, :] = x

    leave = [
        pltpu.make_async_copy(sol_ref, sol_hbm, sems.at[0]),
        pltpu.make_async_copy(res_ref, res_hbm, sems.at[1]),
    ]
    combine(res, res_ref)
    leave[1].start()
    combine(sol, sol_ref)
    leave[0].start()
    leave[1].wait()
    leave[0].wait()


def by_rows(array):
    return array.reshape(array.shape[0], -1, LZ).transpose(1, 0, 2)


def stay(array):
    return pltpu.with_memory_space_constraint(array, pltpu.HBM)


def on_device(positions, radii, neighbours, right_side):
    owned = positions.shape[1]
    rows = owned // LZ
    devices = lax.axis_size("gx")
    place = lax.axis_index("gx").astype(jnp.int32)
    first = (place * owned).reshape(1)
    odd = (place % 2).reshape(1)
    vmem = pl.BlockSpec(memory_space=pltpu.VMEM)
    smem = pl.BlockSpec(memory_space=pltpu.SMEM)
    hbm = pl.BlockSpec(memory_space=pltpu.HBM)

    packed = pl.pallas_call(
        pack_kernel,
        out_shape=jax.ShapeDtypeStruct((10, rows, LZ), f32),
        in_specs=[smem, hbm, hbm, hbm, hbm],
        out_specs=vmem,
        scratch_shapes=[
            pltpu.VMEM((rows, 3, LZ), f32),
            pltpu.VMEM((rows, LZ), f32),
            pltpu.VMEM((rows, neighbours.shape[0], LZ), jnp.int32),
            pltpu.VMEM((rows, 3, LZ), f32),
            pltpu.SemaphoreType.DMA((4,)),
        ],
        compiler_params=pltpu.CompilerParams(vmem_limit_bytes=4 << 20),
        name="pack",
    )(
        first,
        stay(by_rows(positions)),
        stay(radii.reshape(rows, LZ)),
        stay(by_rows(neighbours)),
        stay(by_rows(right_side)),
    )

    def moved(array, to):
        return lax.ppermute(array, "gx", [(i, to(i) % devices) for i in range(devices)])

    low, high = pl.pallas_call(
        edge_kernel,
        out_shape=(
            jax.ShapeDtypeStruct((10, LY, LZ), f32),
            jax.ShapeDtypeStruct((12, LY, LZ), f32),
        ),
        in_specs=[vmem],
        out_specs=(vmem, vmem),
        compiler_params=pltpu.CompilerParams(vmem_limit_bytes=4 << 20),
        name="edge",
    )(packed)
    across = moved(packed, lambda i: i + 1 if i % 2 else i - 1)
    far_left = moved(high, lambda i: i + 2)
    far_right = moved(low, lambda i: i - 2)
    mate = moved(packed, lambda i: i ^ 1)

    basis, sums = pl.pallas_call(
        krylov_kernel,
        out_shape=(
            jax.ShapeDtypeStruct((3 * (ITERS + 1), rows, LZ), f32),
            jax.ShapeDtypeStruct((1, LZ), f32),
        ),
        in_specs=[smem] + [vmem] * 5,
        out_specs=(vmem, vmem),
        compiler_params=pltpu.CompilerParams(vmem_limit_bytes=12 << 20),
        name="krylov",
    )(odd, far_left, across, packed, mate, far_right)

    chips = devices // 2
    sums = sums + moved(sums, lambda i: i ^ 1)
    groups = [[2 * ((z + chips // 2) % chips) + c for z in range(chips)] for c in (0, 1)]
    everyone = lax.all_to_all(
        jnp.broadcast_to(sums[None], (chips, 1, LZ)),
        "gx",
        split_axis=0,
        concat_axis=0,
        tiled=True,
        axis_index_groups=groups,
    )

    sol, res = pl.pallas_call(
        finish_kernel,
        out_shape=(
            jax.ShapeDtypeStruct((rows, 3, LZ), f32),
            jax.ShapeDtypeStruct((rows, 3, LZ), f32),
        ),
        in_specs=[vmem, vmem],
        out_specs=(hbm, hbm),
        scratch_shapes=[
            pltpu.VMEM((rows, 3, LZ), f32),
            pltpu.VMEM((rows, 3, LZ), f32),
            pltpu.SemaphoreType.DMA((2,)),
        ],
        compiler_params=pltpu.CompilerParams(vmem_limit_bytes=4 << 20),
        name="finish",
    )(basis, everyone.reshape(-1, 8, LZ))
    back = lambda a: a.transpose(1, 0, 2).reshape(3, owned)
    return back(sol), back(res)


def solution(mesh):
    return jax.shard_map(
        on_device,
        mesh=mesh,
        in_specs=(
            P(None, ("groups", "gx")),
            P(("groups", "gx")),
            P(None, ("groups", "gx")),
            P(None, ("groups", "gx")),
        ),
        out_specs=(P(None, ("groups", "gx")), P(None, ("groups", "gx"))),
        check_vma=False,
    )
```

```python
import jax
import jax.numpy as jnp
from jax import lax
from jax.experimental import pallas as pl
from jax.experimental.pallas import tpu as pltpu
from jax.sharding import PartitionSpec as P


LY = 16
LZ = 128
ITERS = 4
DIAGONAL_SHIFT = 4.0

CENTER = 5.7
RADIUS = 2.3
STILL = (DIAGONAL_SHIFT - CENTER) / RADIUS
ORIGIN = -CENTER / RADIUS
MOMENTS = 2 * ITERS

f32 = jnp.float32


def first_kind(order, at):
    below, value = at, 1.0
    for _ in range(order):
        below, value = value, 2.0 * at * value - below
    return value


def quotient(order, at):
    second = [1.0, 2.0 * at]
    while len(second) < order:
        second.append(2.0 * at * second[-1] - second[-2])
    return [(1.0 if i == 0 else 2.0) * second[order - 1 - i] for i in range(order)]


def pack_kernel(
    first_ref, pos_hbm, rad_hbm, nb_hbm, rhs_hbm, out_ref, low_ref, high_ref, *scratch
):
    pos_ref, rad_ref, nb_ref, rhs_ref, sems = scratch
    moves = [
        pltpu.make_async_copy(src, dst, sems.at[k])
        for k, (src, dst) in enumerate(
            (
                (nb_hbm, nb_ref),
                (pos_hbm, pos_ref),
                (rhs_hbm, rhs_ref),
                (rad_hbm, rad_ref),
            )
        )
    ]
    for move in moves:
        move.start()
    rows = rad_ref.shape[0]
    shape = (rows, LZ)
    ids = first_ref[0] + (
        lax.broadcasted_iota(jnp.int32, shape, 0) * LZ
        + lax.broadcasted_iota(jnp.int32, shape, 1)
    )
    for move in moves[1:]:
        move.wait()
    for c in range(3):
        out_ref[c] = pos_ref[:, c, :]
        out_ref[7 + c] = rhs_ref[:, c, :]
    out_ref[3] = rad_ref[...]
    moves[0].wait()
    slots = [nb_ref[:, s, :] - ids for s in range(nb_ref.shape[1])]
    for b, shift in enumerate((LY * LZ, LZ, 1)):
        hit = slots[0] == shift
        for other in slots[1:]:
            hit = hit | (other == shift)
        out_ref[4 + b] = jnp.where(hit, f32(1.0), f32(0.0))
    write_edges(out_ref, low_ref, high_ref)


def write_edges(own_ref, low_ref, high_ref):
    rows = own_ref.shape[1]
    row, lane = coordinates(rows)
    geom = [own_ref[c] for c in range(4)]
    inside = row < rows - 1
    last = (row == rows - 1) & (lane == LZ - 1)
    vector = [own_ref[7 + c] for c in range(3)]
    bonds = all_bonds(
        geom,
        [own_ref[4], own_ref[5], own_ref[6]],
        lane,
        (None, inside, jnp.logical_not(last)),
    )
    push = fluxes(bonds, vector, lane, 0, rows)
    for c in range(3):
        low_ref[c] = geom[c][:LY]
        high_ref[c] = geom[c][rows - LY :]
        low_ref[4 + c] = vector[c][:LY]
        high_ref[4 + c] = vector[c][rows - LY :]
        low_ref[7 + c] = push[c][:LY]
        high_ref[7 + c] = push[c][rows - LY :]
    low_ref[3] = geom[3][:LY]
    high_ref[3] = geom[3][rows - LY :]
    high_ref[10] = own_ref[4, rows - LY :, :]
    high_ref[11, : LY // 2, :] = own_ref[5, rows - LY // 2 :, :]
    high_ref[11, LY // 2 :, :] = own_ref[6, rows - LY // 2 :, :]


def coordinates(rows):
    shape = (rows, LZ)
    return (
        lax.broadcasted_iota(jnp.int32, shape, 0),
        lax.broadcasted_iota(jnp.int32, shape, 1),
    )


def up_row(x):
    return pltpu.roll(x, x.shape[0] - 1, 0)


def down_row(x):
    return pltpu.roll(x, 1, 0)


def next_lane(x, x_up, lane):
    return pltpu.roll(jnp.where(lane == 0, x_up, x), LZ - 1, 1)


def bond(mask, delta, contact, allowed=None):
    if allowed is not None:
        mask = jnp.where(allowed, mask, f32(0.0))
    squared = delta[0] * delta[0] + delta[1] * delta[1] + delta[2] * delta[2]
    shrink = lax.rsqrt(squared)
    inverse = 1.0 / (contact * (squared * shrink))
    scaled = inverse * f32(2.0 / RADIUS)
    present = scaled * mask
    tension = (squared * inverse - 1.0) * present
    weight = (present * lax.rsqrt(scaled)) * shrink
    return tension, [d * weight for d in delta]


def all_bonds(geom, masks, lane, allowed=(None, None, None)):
    total = geom[0].shape[0]
    ahead = [g[LY:] for g in geom]
    base = [g[: total - LY] for g in geom]
    ups = [up_row(g) for g in geom]
    nexts = [next_lane(g, u, lane) for g, u in zip(geom, ups)]

    def build(mask, there, here, ok):
        delta = [a - b for a, b in zip(there[:3], here[:3])]
        return bond(mask, delta, there[3] + here[3], ok)

    return (
        build(masks[0][: total - LY], ahead, base, allowed[0]),
        build(masks[1], ups, geom, allowed[1]),
        build(masks[2], nexts, geom, allowed[2]),
    )


def flux(pair, here, there):
    tension, w = pair
    rel = [a - b for a, b in zip(here, there)]
    along = w[0] * rel[0] + w[1] * rel[1] + w[2] * rel[2]
    return [tension * r + along * n for r, n in zip(rel, w)]


def cut(values, lo, hi):
    return [v[lo:hi] for v in values]


def cut_pair(pair, lo, hi):
    return pair[0][lo:hi], cut(pair[1], lo, hi)


def side_flux(bonds, mid, up, lane, lo, hi):
    fy = flux(cut_pair(bonds[1], lo, hi), mid, up)
    nxt = [next_lane(x, u, lane) for x, u in zip(mid, up)]
    fz = flux(cut_pair(bonds[2], lo, hi), mid, nxt)
    first = lane == 0
    result = []
    for y, z in zip(fy, fz):
        rolled = pltpu.roll(z, 1, 1)
        back = down_row(y + jnp.where(first, rolled, f32(0.0)))
        result.append(y + z - back - jnp.where(first, f32(0.0), rolled))
    return result


def fluxes(bonds, v, lane, lo, hi):
    n = hi - lo
    fx = flux(cut_pair(bonds[0], lo, hi - LY), cut(v, 0, n - LY), cut(v, LY, n))
    side = side_flux(bonds, v, [up_row(x) for x in v], lane[:n], lo, hi)
    result = []
    for s, x in zip(side, fx):
        parts = [x[:LY], -x[n - 2 * LY :]]
        if n > 2 * LY:
            parts.insert(1, x[LY:] - x[: n - 2 * LY])
        result.append(s + jnp.concatenate(parts, axis=0))
    return result


def krylov_kernel(
    odd_ref, ll_ref, far_ref, own_ref, mate_ref, rr_ref, basis_ref, sums_ref
):
    rows = own_ref.shape[1]
    odd = odd_ref[0] == 1
    depth = rows + LY
    total = rows + 2 * depth
    row, lane = coordinates(total)
    half = LY // 2

    def ext(c, low, high):
        outer, mate = far_ref[c], mate_ref[c]
        left = jnp.where(odd, mate, outer)
        right = jnp.where(odd, outer, mate)
        return jnp.concatenate([low, left, own_ref[c], right, high], axis=0)

    none = jnp.zeros((LY, LZ), f32)
    pad = jnp.zeros((LY - half, LZ), f32)
    rim = row[:half] == half - 1
    corner = rim & (lane[:half] == LZ - 1)
    low_y = jnp.where(rim, ll_ref[11, :half, :], f32(0.0))
    low_z = jnp.where(corner, ll_ref[11, half:, :], f32(0.0))
    geom = [ext(c, ll_ref[c], rr_ref[c]) for c in range(4)]
    vector = [ext(7 + c, ll_ref[4 + c], rr_ref[4 + c]) for c in range(3)]
    masks = [
        ext(4, ll_ref[10], none),
        ext(5, jnp.concatenate([pad, low_y], axis=0), none),
        ext(6, jnp.concatenate([pad, low_z], axis=0), none),
    ]
    bonds = all_bonds(geom, masks, lane)

    def operate(v, lo, hi):
        n = hi - lo
        m = n - 2 * LY
        fx = flux(cut_pair(bonds[0], lo, hi - LY), cut(v, 0, n - LY), cut(v, LY, n))
        up = [up_row(x[8 : n - 8])[: n - 24] for x in v]
        mid = cut(v, 8, n - LY)
        side = side_flux(bonds, mid, up, lane[: n - 24], lo + 8, hi - LY)
        return [
            f32(2.0 * (DIAGONAL_SHIFT - CENTER) / RADIUS) * v[c][LY : LY + m]
            + (fx[c][LY : LY + m] - fx[c][:m])
            + side[c][8 : 8 + m]
            for c in range(3)
        ]

    kept = [cut(vector, depth, depth + rows)]
    push = fluxes(bonds, vector, lane, 0, total)
    lo, hi = 0, total
    before, now = None, []
    for c in range(3):
        given = [ll_ref[7 + c], jnp.zeros((total - 2 * LY, LZ), f32), rr_ref[7 + c]]
        now.append(push[c] + jnp.concatenate(given, axis=0))
    kept.append(cut(now, depth, depth + rows))
    for k in range(1, ITERS):
        image = operate(now, lo, hi)
        m = hi - lo - 2 * LY
        if k == 1:
            after = [f32(0.5) * x for x in image]
        else:
            after = [x - p for x, p in zip(image, cut(before, LY, LY + m))]
        before, now = cut(now, LY, LY + m), after
        lo, hi = lo + LY, hi - LY
        kept.append(cut(now, depth - lo, depth - lo + rows))
    for k in range(ITERS + 1):
        for c in range(3):
            basis_ref[3 * k + c] = kept[k][c]

    sub = lax.broadcasted_iota(jnp.int32, (8, LZ), 0)
    col = lax.broadcasted_iota(jnp.int32, (8, LZ), 1)
    line = jnp.zeros((8, LZ), f32)
    for k in range(MOMENTS):
        i = k // 2
        j = k - i
        prod = (
            kept[i][0] * kept[j][0] + kept[i][1] * kept[j][1] + kept[i][2] * kept[j][2]
        )
        part = prod[:8]
        for r in range(8, rows, 8):
            part = part + prod[r : r + 8]
        for s in (4, 2, 1):
            part = part + pltpu.roll(part, s, 0)
        line = jnp.where(sub == k, part, line)
    for s in (64, 32, 16):
        line = line + pltpu.roll(line, s, 1)
    line = jnp.where(col // 16 == sub, line, f32(0.0))
    for s in (4, 2, 1):
        line = line + pltpu.roll(line, s, 0)
    sums_ref[...] = line[:1]


def coefficients(products):
    size = ITERS + 1
    zero = jnp.zeros_like(products[0])
    nu = list(products[2:4])
    for k in range(2, MOMENTS - 2):
        nu.append(2.0 * products[2 + k] - nu[k % 2])
    gram = [[None] * size for _ in range(size)]
    gram[0][0] = products[0]
    for k in range(1, size):
        value = products[1] * f32(first_kind(k - 1, STILL))
        for i, q in enumerate(quotient(k - 1, STILL) if k > 1 else ()):
            value = value + nu[i] * f32(0.5 * q)
        gram[0][k] = value
    for i in range(1, ITERS):
        for j in range(i, size):
            gram[i][j] = 0.5 * (nu[i + j - 2] + nu[j - i])
    scale = [gram[i][i] * f32(1e-8) for i in range(ITERS)]
    lower = [[None] * ITERS for _ in range(size)]
    for i in range(ITERS):
        pivot = gram[i][i]
        inverse = 1.0 / pivot
        if i:
            inverse = jnp.where(pivot > scale[i], inverse, zero)
        for j in range(i + 1, size):
            lower[j][i] = gram[i][j] * inverse
        for k in range(i + 1, ITERS):
            for j in range(k, size):
                gram[k][j] = gram[k][j] - lower[k][i] * gram[i][j]
    res = [None] * ITERS + [zero + 1.0]
    for i in reversed(range(ITERS)):
        value = lower[ITERS][i]
        for j in range(i + 1, ITERS):
            value = value + lower[j][i] * res[j]
        res[i] = -value
    at_origin = res[0]
    for k in range(1, size):
        weight = -2.0 * DIAGONAL_SHIFT / RADIUS * first_kind(k - 1, ORIGIN)
        at_origin = at_origin + res[k] * f32(weight)
    unit = 1.0 / at_origin
    res = [x * unit for x in res]
    sol = [zero] * ITERS
    for j in range(1, size):
        sol[0] = sol[0] - res[j] * f32(2.0 / RADIUS * first_kind(j - 1, ORIGIN))
        for i, q in enumerate(quotient(j - 1, ORIGIN) if j > 1 else ()):
            sol[i + 1] = sol[i + 1] - res[j] * f32(q / RADIUS)
    return res, sol


def finish_kernel(
    basis_ref, sums_ref, sol_hbm, res_hbm, sol_ref, res_ref, sems
):
    line = jnp.sum(sums_ref[...], axis=0)
    line = jnp.sum(line, axis=0, keepdims=True)
    line = jnp.broadcast_to(line, (8, LZ))
    for s in (8, 4, 2, 1):
        line = line + pltpu.roll(line, s, 1)
    products = [
        jnp.broadcast_to(line[:, 16 * k + 15 : 16 * k + 16], (8, LZ))
        for k in range(MOMENTS)
    ]
    res, sol = coefficients(products)
    rows = basis_ref.shape[1]

    def combine(weights, to_ref):
        for c in range(3):
            for r in range(0, rows, 8):
                x = weights[0] * basis_ref[c, r : r + 8, :]
                for k in range(1, len(weights)):
                    x = x + weights[k] * basis_ref[3 * k + c, r : r + 8, :]
                to_ref[r : r + 8, c, :] = x

    leave = [
        pltpu.make_async_copy(sol_ref, sol_hbm, sems.at[0]),
        pltpu.make_async_copy(res_ref, res_hbm, sems.at[1]),
    ]
    combine(res, res_ref)
    leave[1].start()
    combine(sol, sol_ref)
    leave[0].start()
    leave[1].wait()
    leave[0].wait()


def by_rows(array):
    return array.reshape(array.shape[0], -1, LZ).transpose(1, 0, 2)


def stay(array):
    return pltpu.with_memory_space_constraint(array, pltpu.HBM)


def on_device(positions, radii, neighbours, right_side):
    owned = positions.shape[1]
    rows = owned // LZ
    devices = lax.axis_size("gx")
    place = lax.axis_index("gx").astype(jnp.int32)
    first = (place * owned).reshape(1)
    odd = (place % 2).reshape(1)
    vmem = pl.BlockSpec(memory_space=pltpu.VMEM)
    smem = pl.BlockSpec(memory_space=pltpu.SMEM)
    hbm = pl.BlockSpec(memory_space=pltpu.HBM)

    packed, low, high = pl.pallas_call(
        pack_kernel,
        out_shape=(
            jax.ShapeDtypeStruct((10, rows, LZ), f32),
            jax.ShapeDtypeStruct((10, LY, LZ), f32),
            jax.ShapeDtypeStruct((12, LY, LZ), f32),
        ),
        in_specs=[smem, hbm, hbm, hbm, hbm],
        out_specs=(vmem,) * 3,
        scratch_shapes=[
            pltpu.VMEM((rows, 3, LZ), f32),
            pltpu.VMEM((rows, LZ), f32),
            pltpu.VMEM((rows, neighbours.shape[0], LZ), jnp.int32),
            pltpu.VMEM((rows, 3, LZ), f32),
            pltpu.SemaphoreType.DMA((4,)),
        ],
        compiler_params=pltpu.CompilerParams(vmem_limit_bytes=4 << 20),
        name="pack",
    )(
        first,
        stay(by_rows(positions)),
        stay(radii.reshape(rows, LZ)),
        stay(by_rows(neighbours)),
        stay(by_rows(right_side)),
    )

    def moved(array, to):
        return lax.ppermute(array, "gx", [(i, to(i) % devices) for i in range(devices)])

    across = moved(packed, lambda i: i + 1 if i % 2 else i - 1)
    far_left = moved(high, lambda i: i + 2)
    far_right = moved(low, lambda i: i - 2)
    mate = moved(packed, lambda i: i ^ 1)

    basis, sums = pl.pallas_call(
        krylov_kernel,
        out_shape=(
            jax.ShapeDtypeStruct((3 * (ITERS + 1), rows, LZ), f32),
            jax.ShapeDtypeStruct((1, LZ), f32),
        ),
        in_specs=[smem] + [vmem] * 5,
        out_specs=(vmem, vmem),
        compiler_params=pltpu.CompilerParams(vmem_limit_bytes=12 << 20),
        name="krylov",
    )(odd, far_left, across, packed, mate, far_right)

    chips = devices // 2
    sums = sums + moved(sums, lambda i: i ^ 1)
    groups = [[2 * ((z + chips // 2) % chips) + c for z in range(chips)] for c in (0, 1)]
    everyone = lax.all_to_all(
        jnp.broadcast_to(sums[None], (chips, 1, LZ)),
        "gx",
        split_axis=0,
        concat_axis=0,
        tiled=True,
        axis_index_groups=groups,
    )

    sol, res = pl.pallas_call(
        finish_kernel,
        out_shape=(
            jax.ShapeDtypeStruct((rows, 3, LZ), f32),
            jax.ShapeDtypeStruct((rows, 3, LZ), f32),
        ),
        in_specs=[vmem, vmem],
        out_specs=(hbm, hbm),
        scratch_shapes=[
            pltpu.VMEM((rows, 3, LZ), f32),
            pltpu.VMEM((rows, 3, LZ), f32),
            pltpu.SemaphoreType.DMA((2,)),
        ],
        compiler_params=pltpu.CompilerParams(vmem_limit_bytes=4 << 20),
        name="finish",
    )(basis, everyone.reshape(-1, 8, LZ))
    back = lambda a: a.transpose(1, 0, 2).reshape(3, owned)
    return back(sol), back(res)


def solution(mesh):
    return jax.shard_map(
        on_device,
        mesh=mesh,
        in_specs=(
            P(None, ("groups", "gx")),
            P(("groups", "gx")),
            P(None, ("groups", "gx")),
            P(None, ("groups", "gx")),
        ),
        out_specs=(P(None, ("groups", "gx")), P(None, ("groups", "gx"))),
        check_vma=False,
    )
```

```python
import jax
import jax.numpy as jnp
from jax import lax
from jax.experimental import pallas as pl
from jax.experimental.pallas import tpu as pltpu
from jax.sharding import PartitionSpec as P


LY = 16
LZ = 128
ITERS = 4
DIAGONAL_SHIFT = 4.0

CENTER = 5.7
RADIUS = 2.3
STILL = (DIAGONAL_SHIFT - CENTER) / RADIUS
ORIGIN = -CENTER / RADIUS
MOMENTS = 2 * ITERS

f32 = jnp.float32


def first_kind(order, at):
    below, value = at, 1.0
    for _ in range(order):
        below, value = value, 2.0 * at * value - below
    return value


def quotient(order, at):
    second = [1.0, 2.0 * at]
    while len(second) < order:
        second.append(2.0 * at * second[-1] - second[-2])
    return [(1.0 if i == 0 else 2.0) * second[order - 1 - i] for i in range(order)]


def pack_kernel(
    first_ref, pos_hbm, rad_hbm, nb_hbm, rhs_hbm, out_ref, low_ref, high_ref, *scratch
):
    pos_ref, rad_ref, nb_ref, rhs_ref, sems = scratch
    moves = [
        pltpu.make_async_copy(src, dst, sems.at[k])
        for k, (src, dst) in enumerate(
            (
                (nb_hbm, nb_ref),
                (pos_hbm, pos_ref),
                (rhs_hbm, rhs_ref),
                (rad_hbm, rad_ref),
            )
        )
    ]
    for move in moves:
        move.start()
    rows = rad_ref.shape[0]
    shape = (rows, LZ)
    ids = first_ref[0] + (
        lax.broadcasted_iota(jnp.int32, shape, 0) * LZ
        + lax.broadcasted_iota(jnp.int32, shape, 1)
    )
    for move in moves[1:]:
        move.wait()
    for c in range(3):
        out_ref[c] = pos_ref[:, c, :]
        out_ref[7 + c] = rhs_ref[:, c, :]
    out_ref[3] = rad_ref[...]
    moves[0].wait()
    slots = [nb_ref[:, s, :] - ids for s in range(nb_ref.shape[1])]
    for b, shift in enumerate((LY * LZ, LZ, 1)):
        hit = slots[0] == shift
        for other in slots[1:]:
            hit = hit | (other == shift)
        out_ref[4 + b] = jnp.where(hit, f32(1.0), f32(0.0))
    write_edges(out_ref, low_ref, high_ref)


def write_edges(own_ref, low_ref, high_ref):
    rows = own_ref.shape[1]
    row, lane = coordinates(rows)
    geom = [own_ref[c] for c in range(4)]
    inside = row < rows - 1
    last = (row == rows - 1) & (lane == LZ - 1)
    vector = [own_ref[7 + c] for c in range(3)]
    bonds = all_bonds(
        geom,
        [own_ref[4], own_ref[5], own_ref[6]],
        lane,
        (None, inside, jnp.logical_not(last)),
    )
    push = fluxes(bonds, vector, lane, 0, rows)
    for c in range(3):
        low_ref[c] = geom[c][:LY]
        high_ref[c] = geom[c][rows - LY :]
        low_ref[4 + c] = vector[c][:LY]
        high_ref[4 + c] = vector[c][rows - LY :]
        low_ref[7 + c] = push[c][:LY]
        high_ref[7 + c] = push[c][rows - LY :]
    low_ref[3] = geom[3][:LY]
    high_ref[3] = geom[3][rows - LY :]
    high_ref[10] = own_ref[4, rows - LY :, :]
    high_ref[11, : LY // 2, :] = own_ref[5, rows - LY // 2 :, :]
    high_ref[11, LY // 2 :, :] = own_ref[6, rows - LY // 2 :, :]


def coordinates(rows):
    shape = (rows, LZ)
    return (
        lax.broadcasted_iota(jnp.int32, shape, 0),
        lax.broadcasted_iota(jnp.int32, shape, 1),
    )


def up_row(x):
    return pltpu.roll(x, x.shape[0] - 1, 0)


def down_row(x):
    return pltpu.roll(x, 1, 0)


def next_lane(x, x_up, lane):
    return pltpu.roll(jnp.where(lane == 0, x_up, x), LZ - 1, 1)


def bond(mask, delta, contact, allowed=None):
    if allowed is not None:
        mask = jnp.where(allowed, mask, f32(0.0))
    squared = delta[0] * delta[0] + delta[1] * delta[1] + delta[2] * delta[2]
    shrink = lax.rsqrt(squared)
    inverse = 1.0 / (contact * (squared * shrink))
    scaled = inverse * f32(2.0 / RADIUS)
    present = scaled * mask
    tension = (squared * inverse - 1.0) * present
    weight = (present * lax.rsqrt(scaled)) * shrink
    return tension, [d * weight for d in delta]


def all_bonds(geom, masks, lane, allowed=(None, None, None)):
    total = geom[0].shape[0]
    ahead = [g[LY:] for g in geom]
    base = [g[: total - LY] for g in geom]
    ups = [up_row(g) for g in geom]
    nexts = [next_lane(g, u, lane) for g, u in zip(geom, ups)]

    def build(mask, there, here, ok):
        delta = [a - b for a, b in zip(there[:3], here[:3])]
        return bond(mask, delta, there[3] + here[3], ok)

    return (
        build(masks[0][: total - LY], ahead, base, allowed[0]),
        build(masks[1], ups, geom, allowed[1]),
        build(masks[2], nexts, geom, allowed[2]),
    )


def flux(pair, here, there):
    tension, w = pair
    rel = [a - b for a, b in zip(here, there)]
    along = w[0] * rel[0] + w[1] * rel[1] + w[2] * rel[2]
    return [tension * r + along * n for r, n in zip(rel, w)]


def cut(values, lo, hi):
    return [v[lo:hi] for v in values]


def cut_pair(pair, lo, hi):
    return pair[0][lo:hi], cut(pair[1], lo, hi)


def side_flux(bonds, mid, up, lane, lo, hi):
    fy = flux(cut_pair(bonds[1], lo, hi), mid, up)
    nxt = [next_lane(x, u, lane) for x, u in zip(mid, up)]
    fz = flux(cut_pair(bonds[2], lo, hi), mid, nxt)
    first = lane == 0
    result = []
    for y, z in zip(fy, fz):
        rolled = pltpu.roll(z, 1, 1)
        back = down_row(y + jnp.where(first, rolled, f32(0.0)))
        result.append(y + z - back - jnp.where(first, f32(0.0), rolled))
    return result


def fluxes(bonds, v, lane, lo, hi):
    n = hi - lo
    fx = flux(cut_pair(bonds[0], lo, hi - LY), cut(v, 0, n - LY), cut(v, LY, n))
    side = side_flux(bonds, v, [up_row(x) for x in v], lane[:n], lo, hi)
    result = []
    for s, x in zip(side, fx):
        parts = [x[:LY], -x[n - 2 * LY :]]
        if n > 2 * LY:
            parts.insert(1, x[LY:] - x[: n - 2 * LY])
        result.append(s + jnp.concatenate(parts, axis=0))
    return result


def krylov_kernel(ll_ref, l_ref, own_ref, r_ref, rr_ref, basis_ref, sums_ref):
    rows = own_ref.shape[1]
    depth = rows + LY
    total = rows + 2 * depth
    row, lane = coordinates(total)
    half = LY // 2

    def ext(c, low, high):
        return jnp.concatenate([low, l_ref[c], own_ref[c], r_ref[c], high], axis=0)

    none = jnp.zeros((LY, LZ), f32)
    pad = jnp.zeros((LY - half, LZ), f32)
    rim = row[:half] == half - 1
    corner = rim & (lane[:half] == LZ - 1)
    low_y = jnp.where(rim, ll_ref[11, :half, :], f32(0.0))
    low_z = jnp.where(corner, ll_ref[11, half:, :], f32(0.0))
    geom = [ext(c, ll_ref[c], rr_ref[c]) for c in range(4)]
    vector = [ext(7 + c, ll_ref[4 + c], rr_ref[4 + c]) for c in range(3)]
    masks = [
        ext(4, ll_ref[10], none),
        ext(5, jnp.concatenate([pad, low_y], axis=0), none),
        ext(6, jnp.concatenate([pad, low_z], axis=0), none),
    ]
    bonds = all_bonds(geom, masks, lane)

    def operate(v, lo, hi):
        n = hi - lo
        m = n - 2 * LY
        fx = flux(cut_pair(bonds[0], lo, hi - LY), cut(v, 0, n - LY), cut(v, LY, n))
        up = [up_row(x[8 : n - 8])[: n - 24] for x in v]
        mid = cut(v, 8, n - LY)
        side = side_flux(bonds, mid, up, lane[: n - 24], lo + 8, hi - LY)
        return [
            f32(2.0 * (DIAGONAL_SHIFT - CENTER) / RADIUS) * v[c][LY : LY + m]
            + (fx[c][LY : LY + m] - fx[c][:m])
            + side[c][8 : 8 + m]
            for c in range(3)
        ]

    kept = [cut(vector, depth, depth + rows)]
    push = fluxes(bonds, vector, lane, 0, total)
    lo, hi = 0, total
    before, now = None, []
    for c in range(3):
        given = [ll_ref[7 + c], jnp.zeros((total - 2 * LY, LZ), f32), rr_ref[7 + c]]
        now.append(push[c] + jnp.concatenate(given, axis=0))
    kept.append(cut(now, depth, depth + rows))
    for k in range(1, ITERS):
        image = operate(now, lo, hi)
        m = hi - lo - 2 * LY
        if k == 1:
            after = [f32(0.5) * x for x in image]
        else:
            after = [x - p for x, p in zip(image, cut(before, LY, LY + m))]
        before, now = cut(now, LY, LY + m), after
        lo, hi = lo + LY, hi - LY
        kept.append(cut(now, depth - lo, depth - lo + rows))
    for k in range(ITERS + 1):
        for c in range(3):
            basis_ref[3 * k + c] = kept[k][c]

    sub = lax.broadcasted_iota(jnp.int32, (8, LZ), 0)
    col = lax.broadcasted_iota(jnp.int32, (8, LZ), 1)
    line = jnp.zeros((8, LZ), f32)
    for k in range(MOMENTS):
        i = k // 2
        j = k - i
        prod = (
            kept[i][0] * kept[j][0] + kept[i][1] * kept[j][1] + kept[i][2] * kept[j][2]
        )
        part = prod[:8]
        for r in range(8, rows, 8):
            part = part + prod[r : r + 8]
        for s in (4, 2, 1):
            part = part + pltpu.roll(part, s, 0)
        line = jnp.where(sub == k, part, line)
    for s in (64, 32, 16):
        line = line + pltpu.roll(line, s, 1)
    line = jnp.where(col // 16 == sub, line, f32(0.0))
    for s in (4, 2, 1):
        line = line + pltpu.roll(line, s, 0)
    sums_ref[...] = line[:1]


def coefficients(products):
    size = ITERS + 1
    zero = jnp.zeros_like(products[0])
    nu = list(products[2:4])
    for k in range(2, MOMENTS - 2):
        nu.append(2.0 * products[2 + k] - nu[k % 2])
    gram = [[None] * size for _ in range(size)]
    gram[0][0] = products[0]
    for k in range(1, size):
        value = products[1] * f32(first_kind(k - 1, STILL))
        for i, q in enumerate(quotient(k - 1, STILL) if k > 1 else ()):
            value = value + nu[i] * f32(0.5 * q)
        gram[0][k] = value
    for i in range(1, ITERS):
        for j in range(i, size):
            gram[i][j] = 0.5 * (nu[i + j - 2] + nu[j - i])
    scale = [gram[i][i] * f32(1e-8) for i in range(ITERS)]
    lower = [[None] * ITERS for _ in range(size)]
    for i in range(ITERS):
        pivot = gram[i][i]
        inverse = 1.0 / pivot
        if i:
            inverse = jnp.where(pivot > scale[i], inverse, zero)
        for j in range(i + 1, size):
            lower[j][i] = gram[i][j] * inverse
        for k in range(i + 1, ITERS):
            for j in range(k, size):
                gram[k][j] = gram[k][j] - lower[k][i] * gram[i][j]
    res = [None] * ITERS + [zero + 1.0]
    for i in reversed(range(ITERS)):
        value = lower[ITERS][i]
        for j in range(i + 1, ITERS):
            value = value + lower[j][i] * res[j]
        res[i] = -value
    at_origin = res[0]
    for k in range(1, size):
        weight = -2.0 * DIAGONAL_SHIFT / RADIUS * first_kind(k - 1, ORIGIN)
        at_origin = at_origin + res[k] * f32(weight)
    unit = 1.0 / at_origin
    res = [x * unit for x in res]
    sol = [zero] * ITERS
    for j in range(1, size):
        sol[0] = sol[0] - res[j] * f32(2.0 / RADIUS * first_kind(j - 1, ORIGIN))
        for i, q in enumerate(quotient(j - 1, ORIGIN) if j > 1 else ()):
            sol[i + 1] = sol[i + 1] - res[j] * f32(q / RADIUS)
    return res, sol


def finish_kernel(
    basis_ref, sums_ref, sol_hbm, res_hbm, sol_ref, res_ref, sems
):
    line = jnp.sum(sums_ref[...], axis=0)
    line = jnp.sum(line, axis=0, keepdims=True)
    line = jnp.broadcast_to(line, (8, LZ))
    for s in (8, 4, 2, 1):
        line = line + pltpu.roll(line, s, 1)
    products = [
        jnp.broadcast_to(line[:, 16 * k + 15 : 16 * k + 16], (8, LZ))
        for k in range(MOMENTS)
    ]
    res, sol = coefficients(products)
    rows = basis_ref.shape[1]

    def combine(weights, to_ref):
        for c in range(3):
            for r in range(0, rows, 8):
                x = weights[0] * basis_ref[c, r : r + 8, :]
                for k in range(1, len(weights)):
                    x = x + weights[k] * basis_ref[3 * k + c, r : r + 8, :]
                to_ref[r : r + 8, c, :] = x

    leave = [
        pltpu.make_async_copy(sol_ref, sol_hbm, sems.at[0]),
        pltpu.make_async_copy(res_ref, res_hbm, sems.at[1]),
    ]
    combine(res, res_ref)
    leave[1].start()
    combine(sol, sol_ref)
    leave[0].start()
    leave[1].wait()
    leave[0].wait()


def by_rows(array):
    return array.reshape(array.shape[0], -1, LZ).transpose(1, 0, 2)


def stay(array):
    return pltpu.with_memory_space_constraint(array, pltpu.HBM)


def on_device(positions, radii, neighbours, right_side):
    owned = positions.shape[1]
    rows = owned // LZ
    devices = lax.axis_size("gx")
    first = (lax.axis_index("gx") * owned).astype(jnp.int32).reshape(1)
    vmem = pl.BlockSpec(memory_space=pltpu.VMEM)
    smem = pl.BlockSpec(memory_space=pltpu.SMEM)
    hbm = pl.BlockSpec(memory_space=pltpu.HBM)

    packed, low, high = pl.pallas_call(
        pack_kernel,
        out_shape=(
            jax.ShapeDtypeStruct((10, rows, LZ), f32),
            jax.ShapeDtypeStruct((10, LY, LZ), f32),
            jax.ShapeDtypeStruct((12, LY, LZ), f32),
        ),
        in_specs=[smem, hbm, hbm, hbm, hbm],
        out_specs=(vmem,) * 3,
        scratch_shapes=[
            pltpu.VMEM((rows, 3, LZ), f32),
            pltpu.VMEM((rows, LZ), f32),
            pltpu.VMEM((rows, neighbours.shape[0], LZ), jnp.int32),
            pltpu.VMEM((rows, 3, LZ), f32),
            pltpu.SemaphoreType.DMA((4,)),
        ],
        compiler_params=pltpu.CompilerParams(vmem_limit_bytes=4 << 20),
        name="pack",
    )(
        first,
        stay(by_rows(positions)),
        stay(radii.reshape(rows, LZ)),
        stay(by_rows(neighbours)),
        stay(by_rows(right_side)),
    )

    def moved(array, to):
        return lax.ppermute(array, "gx", [(i, to(i) % devices) for i in range(devices)])

    left = moved(packed, lambda i: i + 1)
    far_left = moved(high, lambda i: i + 2)
    far_right = moved(low, lambda i: i - 2)
    right = moved(packed, lambda i: i - 1)

    basis, sums = pl.pallas_call(
        krylov_kernel,
        out_shape=(
            jax.ShapeDtypeStruct((3 * (ITERS + 1), rows, LZ), f32),
            jax.ShapeDtypeStruct((1, LZ), f32),
        ),
        in_specs=[vmem] * 5,
        out_specs=(vmem, vmem),
        compiler_params=pltpu.CompilerParams(vmem_limit_bytes=12 << 20),
        name="krylov",
    )(far_left, left, packed, right, far_right)

    chips = devices // 2
    sums = sums + moved(sums, lambda i: i ^ 1)
    groups = [[2 * ((z + chips // 2) % chips) + c for z in range(chips)] for c in (0, 1)]
    everyone = lax.all_to_all(
        jnp.broadcast_to(sums[None], (chips, 1, LZ)),
        "gx",
        split_axis=0,
        concat_axis=0,
        tiled=True,
        axis_index_groups=groups,
    )

    sol, res = pl.pallas_call(
        finish_kernel,
        out_shape=(
            jax.ShapeDtypeStruct((rows, 3, LZ), f32),
            jax.ShapeDtypeStruct((rows, 3, LZ), f32),
        ),
        in_specs=[vmem, vmem],
        out_specs=(hbm, hbm),
        scratch_shapes=[
            pltpu.VMEM((rows, 3, LZ), f32),
            pltpu.VMEM((rows, 3, LZ), f32),
            pltpu.SemaphoreType.DMA((2,)),
        ],
        compiler_params=pltpu.CompilerParams(vmem_limit_bytes=4 << 20),
        name="finish",
    )(basis, everyone.reshape(-1, 8, LZ))
    back = lambda a: a.transpose(1, 0, 2).reshape(3, owned)
    return back(sol), back(res)


def solution(mesh):
    return jax.shard_map(
        on_device,
        mesh=mesh,
        in_specs=(
            P(None, ("groups", "gx")),
            P(("groups", "gx")),
            P(None, ("groups", "gx")),
            P(None, ("groups", "gx")),
        ),
        out_specs=(P(None, ("groups", "gx")), P(None, ("groups", "gx"))),
        check_vma=False,
    )
```

```python
import jax
import jax.numpy as jnp
from jax import lax
from jax.experimental import pallas as pl
from jax.experimental.pallas import tpu as pltpu
from jax.sharding import PartitionSpec as P


LY = 16
LZ = 128
ITERS = 4
DIAGONAL_SHIFT = 4.0

CENTER = 5.7
RADIUS = 2.3
STILL = (DIAGONAL_SHIFT - CENTER) / RADIUS
ORIGIN = -CENTER / RADIUS
MOMENTS = 2 * ITERS

f32 = jnp.float32


def first_kind(order, at):
    below, value = at, 1.0
    for _ in range(order):
        below, value = value, 2.0 * at * value - below
    return value


def quotient(order, at):
    second = [1.0, 2.0 * at]
    while len(second) < order:
        second.append(2.0 * at * second[-1] - second[-2])
    return [(1.0 if i == 0 else 2.0) * second[order - 1 - i] for i in range(order)]


def pack_kernel(
    first_ref, pos_hbm, rad_hbm, nb_hbm, rhs_hbm, out_ref, low_ref, high_ref, *scratch
):
    pos_ref, rad_ref, nb_ref, rhs_ref, sems = scratch
    moves = [
        pltpu.make_async_copy(src, dst, sems.at[k])
        for k, (src, dst) in enumerate(
            (
                (nb_hbm, nb_ref),
                (pos_hbm, pos_ref),
                (rhs_hbm, rhs_ref),
                (rad_hbm, rad_ref),
            )
        )
    ]
    for move in moves:
        move.start()
    rows = rad_ref.shape[0]
    shape = (rows, LZ)
    ids = first_ref[0] + (
        lax.broadcasted_iota(jnp.int32, shape, 0) * LZ
        + lax.broadcasted_iota(jnp.int32, shape, 1)
    )
    for move in moves[1:]:
        move.wait()
    for c in range(3):
        out_ref[c] = pos_ref[:, c, :]
        out_ref[7 + c] = rhs_ref[:, c, :]
    out_ref[3] = rad_ref[...]
    moves[0].wait()
    slots = [nb_ref[:, s, :] - ids for s in range(nb_ref.shape[1])]
    for b, shift in enumerate((LY * LZ, LZ, 1)):
        hit = slots[0] == shift
        for other in slots[1:]:
            hit = hit | (other == shift)
        out_ref[4 + b] = jnp.where(hit, f32(1.0), f32(0.0))
    write_edges(out_ref, low_ref, high_ref)


def write_edges(own_ref, low_ref, high_ref):
    rows = own_ref.shape[1]
    row, lane = coordinates(rows)
    geom = [own_ref[c] for c in range(4)]
    inside = row < rows - 1
    last = (row == rows - 1) & (lane == LZ - 1)
    vector = [own_ref[7 + c] for c in range(3)]
    bonds = all_bonds(
        geom,
        [own_ref[4], own_ref[5], own_ref[6]],
        lane,
        (None, inside, jnp.logical_not(last)),
    )
    push = fluxes(bonds, vector, lane)
    for c in range(3):
        low_ref[c] = geom[c][:LY]
        high_ref[c] = geom[c][rows - LY :]
        low_ref[4 + c] = vector[c][:LY]
        high_ref[4 + c] = vector[c][rows - LY :]
        low_ref[7 + c] = push[c][:LY]
        high_ref[7 + c] = push[c][rows - LY :]
    low_ref[3] = geom[3][:LY]
    high_ref[3] = geom[3][rows - LY :]
    high_ref[10] = own_ref[4, rows - LY :, :]
    high_ref[11, : LY // 2, :] = own_ref[5, rows - LY // 2 :, :]
    high_ref[11, LY // 2 :, :] = own_ref[6, rows - LY // 2 :, :]


def coordinates(rows):
    shape = (rows, LZ)
    return (
        lax.broadcasted_iota(jnp.int32, shape, 0),
        lax.broadcasted_iota(jnp.int32, shape, 1),
    )


def up_row(x):
    return pltpu.roll(x, x.shape[0] - 1, 0)


def down_row(x):
    return pltpu.roll(x, 1, 0)


def next_lane(x, x_up, lane):
    return pltpu.roll(jnp.where(lane == 0, x_up, x), LZ - 1, 1)


def bond(mask, delta, contact, allowed=None):
    if allowed is not None:
        mask = jnp.where(allowed, mask, f32(0.0))
    squared = delta[0] * delta[0] + delta[1] * delta[1] + delta[2] * delta[2]
    shrink = lax.rsqrt(squared)
    inverse = 1.0 / (contact * (squared * shrink))
    scaled = inverse * f32(2.0 / RADIUS)
    present = scaled * mask
    tension = (squared * inverse - 1.0) * present
    weight = (present * lax.rsqrt(scaled)) * shrink
    return tension, [d * weight for d in delta]


def all_bonds(geom, masks, lane, allowed=(None, None, None), rim=0):
    total = geom[0].shape[0]
    ahead = [g[LY:] for g in geom]
    base = [g[: total - LY] for g in geom]
    ups = [up_row(g) for g in geom]
    nexts = [next_lane(g, u, lane) for g, u in zip(geom, ups)]

    def inner(*lists):
        return [cut(values, rim, total - rim) for values in lists]

    def build(mask, there, here, ok):
        delta = [a - b for a, b in zip(there[:3], here[:3])]
        return bond(mask, delta, there[3] + here[3], ok)

    return (
        build(masks[0][: total - LY], ahead, base, allowed[0]),
        build(masks[1][rim : total - rim], *inner(ups, geom), allowed[1]),
        build(masks[2][rim : total - rim], *inner(nexts, geom), allowed[2]),
    )


def flux(pair, here, there):
    tension, w = pair
    rel = [a - b for a, b in zip(here, there)]
    along = w[0] * rel[0] + w[1] * rel[1] + w[2] * rel[2]
    return [tension * r + along * n for r, n in zip(rel, w)]


def cut(values, lo, hi):
    return [v[lo:hi] for v in values]


def cut_pair(pair, lo, hi):
    return pair[0][lo:hi], cut(pair[1], lo, hi)


def side_flux(bonds, mid, up, lane, lo, hi):
    fy = flux(cut_pair(bonds[1], lo, hi), mid, up)
    nxt = [next_lane(x, u, lane) for x, u in zip(mid, up)]
    fz = flux(cut_pair(bonds[2], lo, hi), mid, nxt)
    first = lane == 0
    result = []
    for y, z in zip(fy, fz):
        rolled = pltpu.roll(z, 1, 1)
        back = down_row(y + jnp.where(first, rolled, f32(0.0)))
        result.append(y + z - back - jnp.where(first, f32(0.0), rolled))
    return result


def fluxes(bonds, v, lane, rim=0):
    n = v[0].shape[0]
    fx = flux(bonds[0], cut(v, 0, n - LY), cut(v, LY, n))
    m = n - 2 * rim
    mid = cut(v, rim, n - rim)
    side = side_flux(bonds, mid, [up_row(x) for x in mid], lane[:m], 0, m)
    if rim:
        edge = jnp.zeros((rim, LZ), f32)
        side = [jnp.concatenate([edge, x, edge], axis=0) for x in side]
    result = []
    for s, x in zip(side, fx):
        parts = [x[:LY], -x[n - 2 * LY :]]
        if n > 2 * LY:
            parts.insert(1, x[LY:] - x[: n - 2 * LY])
        result.append(s + jnp.concatenate(parts, axis=0))
    return result


def krylov_kernel(ll_ref, l_ref, own_ref, r_ref, rr_ref, basis_ref, sums_ref):
    rows = own_ref.shape[1]
    depth = rows + LY
    total = rows + 2 * depth
    row, lane = coordinates(total)
    half = LY // 2

    def ext(c, low, high):
        return jnp.concatenate([low, l_ref[c], own_ref[c], r_ref[c], high], axis=0)

    none = jnp.zeros((LY, LZ), f32)
    pad = jnp.zeros((LY - half, LZ), f32)
    rim = row[:half] == half - 1
    corner = rim & (lane[:half] == LZ - 1)
    low_y = jnp.where(rim, ll_ref[11, :half, :], f32(0.0))
    low_z = jnp.where(corner, ll_ref[11, half:, :], f32(0.0))
    geom = [ext(c, ll_ref[c], rr_ref[c]) for c in range(4)]
    vector = [ext(7 + c, ll_ref[4 + c], rr_ref[4 + c]) for c in range(3)]
    masks = [
        ext(4, ll_ref[10], none),
        ext(5, jnp.concatenate([pad, low_y], axis=0), none),
        ext(6, jnp.concatenate([pad, low_z], axis=0), none),
    ]
    bonds = all_bonds(geom, masks, lane, rim=half)

    def operate(v, lo, hi):
        n = hi - lo
        m = n - 2 * LY
        fx = flux(cut_pair(bonds[0], lo, hi - LY), cut(v, 0, n - LY), cut(v, LY, n))
        up = [up_row(x[8 : n - 8])[: n - 24] for x in v]
        mid = cut(v, 8, n - LY)
        side = side_flux(bonds, mid, up, lane[: n - 24], lo, hi - 24)
        return [
            f32(2.0 * (DIAGONAL_SHIFT - CENTER) / RADIUS) * v[c][LY : LY + m]
            + (fx[c][LY : LY + m] - fx[c][:m])
            + side[c][8 : 8 + m]
            for c in range(3)
        ]

    kept = [cut(vector, depth, depth + rows)]
    push = fluxes(bonds, vector, lane, rim=half)
    lo, hi = 0, total
    before, now = None, []
    for c in range(3):
        given = [ll_ref[7 + c], jnp.zeros((total - 2 * LY, LZ), f32), rr_ref[7 + c]]
        now.append(push[c] + jnp.concatenate(given, axis=0))
    kept.append(cut(now, depth, depth + rows))
    for k in range(1, ITERS):
        image = operate(now, lo, hi)
        m = hi - lo - 2 * LY
        if k == 1:
            after = [f32(0.5) * x for x in image]
        else:
            after = [x - p for x, p in zip(image, cut(before, LY, LY + m))]
        before, now = cut(now, LY, LY + m), after
        lo, hi = lo + LY, hi - LY
        kept.append(cut(now, depth - lo, depth - lo + rows))
    for k in range(ITERS + 1):
        for c in range(3):
            basis_ref[3 * k + c] = kept[k][c]

    sub = lax.broadcasted_iota(jnp.int32, (8, LZ), 0)
    col = lax.broadcasted_iota(jnp.int32, (8, LZ), 1)
    line = jnp.zeros((8, LZ), f32)
    for k in range(MOMENTS):
        i = k // 2
        j = k - i
        prod = (
            kept[i][0] * kept[j][0] + kept[i][1] * kept[j][1] + kept[i][2] * kept[j][2]
        )
        part = prod[:8]
        for r in range(8, rows, 8):
            part = part + prod[r : r + 8]
        for s in (4, 2, 1):
            part = part + pltpu.roll(part, s, 0)
        line = jnp.where(sub == k, part, line)
    for s in (64, 32, 16):
        line = line + pltpu.roll(line, s, 1)
    line = jnp.where(col // 16 == sub, line, f32(0.0))
    for s in (4, 2, 1):
        line = line + pltpu.roll(line, s, 0)
    sums_ref[...] = line[:1]


def coefficients(products):
    size = ITERS + 1
    zero = jnp.zeros_like(products[0])
    nu = list(products[2:4])
    for k in range(2, MOMENTS - 2):
        nu.append(2.0 * products[2 + k] - nu[k % 2])
    gram = [[None] * size for _ in range(size)]
    gram[0][0] = products[0]
    for k in range(1, size):
        value = products[1] * f32(first_kind(k - 1, STILL))
        for i, q in enumerate(quotient(k - 1, STILL) if k > 1 else ()):
            value = value + nu[i] * f32(0.5 * q)
        gram[0][k] = value
    for i in range(1, ITERS):
        for j in range(i, size):
            gram[i][j] = 0.5 * (nu[i + j - 2] + nu[j - i])
    scale = [gram[i][i] * f32(1e-8) for i in range(ITERS)]
    lower = [[None] * ITERS for _ in range(size)]
    for i in range(ITERS):
        pivot = gram[i][i]
        inverse = 1.0 / pivot
        if i:
            inverse = jnp.where(pivot > scale[i], inverse, zero)
        for j in range(i + 1, size):
            lower[j][i] = gram[i][j] * inverse
        for k in range(i + 1, ITERS):
            for j in range(k, size):
                gram[k][j] = gram[k][j] - lower[k][i] * gram[i][j]
    res = [None] * ITERS + [zero + 1.0]
    for i in reversed(range(ITERS)):
        value = lower[ITERS][i]
        for j in range(i + 1, ITERS):
            value = value + lower[j][i] * res[j]
        res[i] = -value
    at_origin = res[0]
    for k in range(1, size):
        weight = -2.0 * DIAGONAL_SHIFT / RADIUS * first_kind(k - 1, ORIGIN)
        at_origin = at_origin + res[k] * f32(weight)
    unit = 1.0 / at_origin
    res = [x * unit for x in res]
    sol = [zero] * ITERS
    for j in range(1, size):
        sol[0] = sol[0] - res[j] * f32(2.0 / RADIUS * first_kind(j - 1, ORIGIN))
        for i, q in enumerate(quotient(j - 1, ORIGIN) if j > 1 else ()):
            sol[i + 1] = sol[i + 1] - res[j] * f32(q / RADIUS)
    return res, sol


def finish_kernel(
    basis_ref, sums_ref, sol_hbm, res_hbm, sol_ref, res_ref, sems
):
    line = jnp.sum(sums_ref[...], axis=0)
    line = jnp.sum(line, axis=0, keepdims=True)
    line = jnp.broadcast_to(line, (8, LZ))
    for s in (8, 4, 2, 1):
        line = line + pltpu.roll(line, s, 1)
    products = [
        jnp.broadcast_to(line[:, 16 * k + 15 : 16 * k + 16], (8, LZ))
        for k in range(MOMENTS)
    ]
    res, sol = coefficients(products)
    rows = basis_ref.shape[1]

    def combine(weights, to_ref):
        for c in range(3):
            for r in range(0, rows, 8):
                x = weights[0] * basis_ref[c, r : r + 8, :]
                for k in range(1, len(weights)):
                    x = x + weights[k] * basis_ref[3 * k + c, r : r + 8, :]
                to_ref[r : r + 8, c, :] = x

    leave = [
        pltpu.make_async_copy(sol_ref, sol_hbm, sems.at[0]),
        pltpu.make_async_copy(res_ref, res_hbm, sems.at[1]),
    ]
    combine(res, res_ref)
    leave[1].start()
    combine(sol, sol_ref)
    leave[0].start()
    leave[1].wait()
    leave[0].wait()


def by_rows(array):
    return array.reshape(array.shape[0], -1, LZ).transpose(1, 0, 2)


def stay(array):
    return pltpu.with_memory_space_constraint(array, pltpu.HBM)


def on_device(positions, radii, neighbours, right_side):
    owned = positions.shape[1]
    rows = owned // LZ
    devices = lax.axis_size("gx")
    first = (lax.axis_index("gx") * owned).astype(jnp.int32).reshape(1)
    vmem = pl.BlockSpec(memory_space=pltpu.VMEM)
    smem = pl.BlockSpec(memory_space=pltpu.SMEM)
    hbm = pl.BlockSpec(memory_space=pltpu.HBM)

    packed, low, high = pl.pallas_call(
        pack_kernel,
        out_shape=(
            jax.ShapeDtypeStruct((10, rows, LZ), f32),
            jax.ShapeDtypeStruct((10, LY, LZ), f32),
            jax.ShapeDtypeStruct((12, LY, LZ), f32),
        ),
        in_specs=[smem, hbm, hbm, hbm, hbm],
        out_specs=(vmem,) * 3,
        scratch_shapes=[
            pltpu.VMEM((rows, 3, LZ), f32),
            pltpu.VMEM((rows, LZ), f32),
            pltpu.VMEM((rows, neighbours.shape[0], LZ), jnp.int32),
            pltpu.VMEM((rows, 3, LZ), f32),
            pltpu.SemaphoreType.DMA((4,)),
        ],
        compiler_params=pltpu.CompilerParams(vmem_limit_bytes=4 << 20),
        name="pack",
    )(
        first,
        stay(by_rows(positions)),
        stay(radii.reshape(rows, LZ)),
        stay(by_rows(neighbours)),
        stay(by_rows(right_side)),
    )

    def moved(array, to):
        return lax.ppermute(array, "gx", [(i, to(i) % devices) for i in range(devices)])

    left = moved(packed, lambda i: i + 1)
    far_left = moved(high, lambda i: i + 2)
    far_right = moved(low, lambda i: i - 2)
    right = moved(packed, lambda i: i - 1)

    basis, sums = pl.pallas_call(
        krylov_kernel,
        out_shape=(
            jax.ShapeDtypeStruct((3 * (ITERS + 1), rows, LZ), f32),
            jax.ShapeDtypeStruct((1, LZ), f32),
        ),
        in_specs=[vmem] * 5,
        out_specs=(vmem, vmem),
        compiler_params=pltpu.CompilerParams(vmem_limit_bytes=12 << 20),
        name="krylov",
    )(far_left, left, packed, right, far_right)

    chips = devices // 2
    sums = sums + moved(sums, lambda i: i ^ 1)
    groups = [[2 * ((z + chips * 5 // 8) % chips) + c for z in range(chips)] for c in (0, 1)]
    everyone = lax.all_to_all(
        jnp.broadcast_to(sums[None], (chips, 1, LZ)),
        "gx",
        split_axis=0,
        concat_axis=0,
        tiled=True,
        axis_index_groups=groups,
    )

    sol, res = pl.pallas_call(
        finish_kernel,
        out_shape=(
            jax.ShapeDtypeStruct((rows, 3, LZ), f32),
            jax.ShapeDtypeStruct((rows, 3, LZ), f32),
        ),
        in_specs=[vmem, vmem],
        out_specs=(hbm, hbm),
        scratch_shapes=[
            pltpu.VMEM((rows, 3, LZ), f32),
            pltpu.VMEM((rows, 3, LZ), f32),
            pltpu.SemaphoreType.DMA((2,)),
        ],
        compiler_params=pltpu.CompilerParams(vmem_limit_bytes=4 << 20),
        name="finish",
    )(basis, everyone.reshape(-1, 8, LZ))
    back = lambda a: a.transpose(1, 0, 2).reshape(3, owned)
    return back(sol), back(res)


def solution(mesh):
    return jax.shard_map(
        on_device,
        mesh=mesh,
        in_specs=(
            P(None, ("groups", "gx")),
            P(("groups", "gx")),
            P(None, ("groups", "gx")),
            P(None, ("groups", "gx")),
        ),
        out_specs=(P(None, ("groups", "gx")), P(None, ("groups", "gx"))),
        check_vma=False,
    )
```
